32 devices in a mesh: fsdp: 8 (over z, y), tp: 4 (over x, core).
Axes of the slice: x: 2, y: 2, z: 4, core: 2. Of those that a mesh axis runs over, the one named last changes fastest.
Arguments:
- hidden_in: bfloat16 [1024, 8192], P('fsdp'), may hold values from -6 to 6
- key_grad: bfloat16 [1024, 1024], P('fsdp', 'tp'), may hold values from -2.5 to 2.5
- positions: int32 [1024], P('fsdp'), may hold values from 0 to 1023, as said below
- key_quant: bfloat16 [8704, 1024], P('fsdp', 'tp'), may hold values from -4 to 4
- key_scales: float32 [8704, 8], P('fsdp', 'tp'), may hold values from 0.01 to 0.1
- block_counts: int32 [8], replicated, may hold values from 960 to 1088, as said below
Outputs:
- weight_grad: bfloat16 [8704, 1024], P('fsdp', 'tp')
- input_grad: bfloat16 [1024, 8192], P('fsdp', 'tp')
The draws below stay inside these ranges and needn't reach their ends.
Inputs may be any that keep to these rules, and one draw needn't show every extreme that they name: Index f of fsdp owns the consecutive projection rows from block_counts[0] + ... + block_counts[f-1] on, in its first block_counts[f] slots; the counts sum to 8192, and some index owns exactly 1088 rows. positions count the tokens from the start of their packed document; the first token's document may have begun before the first token, and a document may go on into the next index's tokens.
All inputs are finite; a program needn't handle non-finite values.
Results may differ from the reference program's by a relative error of at most 0.013.
Values may be sent and summed in bfloat16 or wider, within the bound.
A program may use at most 64 MiB of HBM per device.

```python
import math
import jax
import jax.numpy as jnp
from jax import lax

D = 8192
KVH = 8
HD = 128
TOKENS = 1024
SLOTS = 1088
N_FSDP = 8
N_TP = 4


def draw_block_counts(key, part):
    base_count = D // N_FSDP
    extra = SLOTS - base_count
    remain = D - N_FSDP * base_count
    order = jax.random.permutation(jax.random.fold_in(key, 11), N_FSDP)
    places = jnp.arange(N_FSDP, dtype=jnp.int32)
    values = base_count + (places < remain).astype(jnp.int32)
    pair_total = N_FSDP // 2
    amounts = jax.random.randint(jax.random.fold_in(key, 12), (pair_total,), 0, extra, dtype=jnp.int32)
    amounts = amounts.at[0].set(SLOTS - values[0])
    pair_idx = jnp.minimum(places // 2, pair_total - 1)
    signs = jnp.where(places % 2 == 0, 1, -1).astype(jnp.int32)
    moved = jnp.where(places // 2 < pair_total, signs * amounts[pair_idx], 0).astype(jnp.int32)
    values = values + moved
    return jnp.zeros((N_FSDP,), jnp.int32).at[order].set(values)


def draw_positions(key, part):
    token_ids = jnp.arange(TOKENS, dtype=jnp.int32)
    first_len = jax.random.randint(jax.random.fold_in(key, 22), (), TOKENS // 4, TOKENS // 2 + 1, dtype=jnp.int32)
    marks = jax.random.randint(jax.random.fold_in(key, 21), (TOKENS,), 0, 256, dtype=jnp.int32)
    opening = (marks == 0) & (token_ids >= first_len) | (token_ids == first_len)
    starts = jnp.where(opening, token_ids, 0).astype(jnp.int32)
    begins = lax.cummax(starts)
    later = (token_ids - begins).astype(jnp.int32)
    carried = (token_ids + TOKENS - first_len).astype(jnp.int32)
    return jnp.where(token_ids < first_len, carried, later).astype(jnp.int32)


def with_spikes(entries, own_key, source, target, parts, factor):
    def block_of(axis_at):
        return (jnp.arange(entries.shape[axis_at]) // (entries.shape[axis_at] // parts)).reshape((-1,) + (1,) * (entries.ndim - 1 - axis_at))

    near = jax.random.permutation(own_key, parts)[block_of(target)]
    other_side = (block_of(target) + parts // 2) % parts
    return jnp.where((block_of(source) == near) | (block_of(source) == other_side), factor * entries, entries)


def levels(own_key, shape, pieces, low, top_value):
    loudness, own = 1.0, jax.random.fold_in(own_key, 6)
    for position, shards_of in pieces:
        steps = jnp.exp(jax.random.uniform(jax.random.fold_in(own, position), (shards_of,), jnp.float32, low / len(pieces), top_value / len(pieces)))
        loudness = loudness * jnp.repeat(steps, shape[position] // shards_of).reshape([-1 if axis == position else 1 for axis in range(len(shape))])
    return loudness


def scatter_about(key, dims, deviation, most, shards=(), kind=jnp.bfloat16):
    gain = levels(key, dims, shards, -0.22, 0.18) if shards else 1.0
    result = jax.random.normal(key, dims, jnp.float32) * deviation * gain
    return jnp.minimum(jnp.maximum(result, -most), most).astype(kind)


def bell_draw_with(key, dims, scale, limit, cuts, heavy, kind=jnp.bfloat16):
    values = scale * jax.random.normal(key, dims, jnp.float32)
    if cuts:
        values = values * levels(key, dims, cuts, -0.22, 0.18)
    return jnp.clip(with_spikes(values, jax.random.fold_in(key, 3), *heavy), -limit, limit).astype(kind)


def setup_inputs(seed: int = 0) -> dict:
    splits = jax.random.split(jax.random.key(seed), 7)
    hidden_in = bell_draw_with(splits[0], (TOKENS, D), 1.0, 6.0, ((0, 8),), (0, 1, 8, 2.0))
    key_grad = scatter_about(splits[1], (TOKENS, KVH * HD), (TOKENS ** -0.25), 2.5, ((0, 8), (1, 4)))
    positions = draw_positions(jax.random.fold_in(splits[6], 71), 0)
    key_quant = scatter_about(splits[3], (N_FSDP * SLOTS, KVH * HD), 1.0, 4.0, ((0, 8), (1, 4)))
    key_scales = jnp.clip(jnp.exp(math.log(0.1) - 2.3025851 * jax.random.uniform(splits[4], (N_FSDP * SLOTS, KVH), jnp.float32) ** levels(splits[4], (N_FSDP * SLOTS, KVH), ((0, 8), (1, 4)), -0.2, 0.2)), 0.01, 0.1)
    block_counts = draw_block_counts(jax.random.fold_in(splits[6], 71), 0)
    return {"hidden_in": hidden_in, "key_grad": key_grad, "positions": positions, "key_quant": key_quant, "key_scales": key_scales, "block_counts": block_counts}


rope_base = 500000.0


def rotary_backward(key_grad, positions):
    tokens_here = key_grad.shape[0]
    half_dim = HD // 2
    cotangent = key_grad.astype(jnp.float32).reshape(tokens_here, -1, HD)
    freq_idx = jnp.arange(half_dim, dtype=jnp.float32)
    inverse = jnp.exp(-(2.0 * freq_idx / HD) * math.log(rope_base))
    angles = positions.astype(jnp.float32)[:, None] * inverse[None, :]
    cosine = jnp.cos(angles)[:, None, :]
    sine_part = jnp.sin(angles)[:, None, :]
    lower_half = cotangent[..., :half_dim]
    upper_half = cotangent[..., half_dim:]
    back_lower = lower_half * cosine + upper_half * sine_part
    back_upper = upper_half * cosine - lower_half * sine_part
    joined = jnp.concatenate([back_lower, back_upper], axis=-1)
    return joined.reshape(tokens_here, -1).astype(jnp.bfloat16)


def slot_tables(block_counts, slot_count, row_total):
    counts = block_counts.astype(jnp.int32)
    offsets = (jnp.cumsum(counts) - counts).astype(jnp.int32)
    owners_n = counts.shape[0]
    slot_ids = jnp.arange(owners_n * slot_count, dtype=jnp.int32)
    within = slot_ids % slot_count
    live_counts = jnp.broadcast_to(counts[:, None], (owners_n, slot_count)).reshape(-1)
    base_rows = jnp.broadcast_to(offsets[:, None], (owners_n, slot_count)).reshape(-1)
    is_live = within < live_counts
    row_of_slot = jnp.where(is_live, base_rows + within, 0).astype(jnp.int32)
    row_ids = jnp.arange(row_total, dtype=jnp.int32)
    at_or_after = row_ids[:, None] >= offsets[None, :]
    owner_of_row = jnp.sum(at_or_after.astype(jnp.int32), axis=1) - 1
    row_begin = jnp.max(jnp.where(at_or_after, offsets[None, :], 0), axis=1)
    slot_of_row = (owner_of_row * slot_count + row_ids - row_begin).astype(jnp.int32)
    return row_of_slot, is_live, slot_of_row


def reference(hidden_in, key_grad, positions, key_quant, key_scales, block_counts):
    row_of_slot, is_live, slot_of_row = slot_tables(block_counts, SLOTS, D)
    scaled = key_quant.astype(jnp.float32).reshape(-1, KVH, HD) * key_scales[:, :, None]
    weights_slots = scaled.astype(jnp.bfloat16).reshape(-1, KVH * HD)
    weights = jnp.take(weights_slots, slot_of_row, axis=0)
    rotated = rotary_backward(key_grad, positions)
    grad_full = jnp.dot(hidden_in.T, rotated, preferred_element_type=jnp.float32)
    grad_slots = jnp.where(is_live[:, None], jnp.take(grad_full, row_of_slot, axis=0), jnp.zeros((), jnp.float32))
    group_width = KVH * HD // N_TP
    total = jnp.zeros((rotated.shape[0], D), jnp.float32)
    for group in range(N_TP):
        lo_col = group * group_width
        part_rot = rotated[:, lo_col:lo_col + group_width]
        part_w = weights[:, lo_col:lo_col + group_width]
        group_part = jnp.dot(part_rot, part_w.T, preferred_element_type=jnp.float32).astype(jnp.bfloat16)
        total = total + group_part.astype(jnp.float32)
    return grad_slots.astype(jnp.bfloat16), total.astype(jnp.bfloat16)
```

```python
import functools
import math

import jax
import jax.numpy as jnp
from jax import lax
from jax.experimental import pallas as pl
from jax.experimental.pallas import tpu as pltpu
from jax.sharding import PartitionSpec as P

HD = 128
LANES = 128
LINE = 2
LOADS = 4
HIDE_EACH = 2
MESH = pl.DeviceIdType.MESH

rope_base = 500000.0


def offset_range(index, owners_n, row_total, slot_count):
    least_count = 2 * row_total // owners_n - slot_count
    later = owners_n - index
    least = max(index * least_count, row_total - later * slot_count)
    greatest = min(index * slot_count, row_total - later * least_count)
    return least, greatest


def exchange_fits(owners_n, group_total, slot_count, row_total, tokens_here, width):
    if group_total != 2 * LINE or owners_n % group_total or owners_n % LINE or slot_count % (16 * group_total):
        return False
    if tokens_here % LANES or width % LANES or row_total % group_total or (row_total // group_total) % LANES:
        return False
    quarter = slot_count // group_total
    chunk = row_total // group_total
    per_chunk = owners_n // group_total
    if 2 * row_total // owners_n - slot_count < quarter or row_total < 2 * quarter + 4 * LANES:
        return False
    for owner in range(owners_n):
        least, greatest = offset_range(owner, owners_n, row_total, slot_count)
        home = owner // per_chunk
        if greatest - least + quarter + 2 * LANES > row_total:
            return False
        for part in range(group_total):
            reach = range(
                max(0, (least + part * quarter) // chunk),
                min(group_total - 1, (greatest + (part + 1) * quarter - 1) // chunk) + 1,
            )
            allowed = {home}
            if part == 0 and owner % per_chunk == 0:
                allowed.add(home - 1)
            if part == group_total - 1 and owner % per_chunk == per_chunk - 1:
                allowed.add(home + 1)
            if not set(reach) <= allowed:
                return False
    return True


def assemble_kernel(owners_n, group_total, pad, counts_ref, pieces_ref, grad_ref, grad_out, out_ref, rows):
    chunk_at = lax.axis_index("tp")
    chunk = out_ref.shape[1]
    quarter = pieces_ref.shape[1]
    per_chunk = owners_n // group_total
    offsets = []
    offset = jnp.int32(0)
    for owner in range(owners_n):
        offsets.append(offset)
        offset = offset + counts_ref[owner]

    def first_row(owner):
        found = jnp.int32(0)
        for candidate in range(owners_n):
            found = jnp.where(owner == candidate, offsets[candidate], found)
        return found

    limit = rows.shape[0] - quarter

    def place(index, begin):
        rows[pl.ds(jnp.clip(begin, 0, limit), quarter), :] = pieces_ref[index].astype(jnp.float32)

    for part in range(group_total):
        grad_out[pl.ds(part * quarter, quarter), :] = grad_ref[part]
    origin = pad - chunk_at * chunk
    first = chunk_at * per_chunk
    below = first_row(first - 1) + (group_total - 1) * quarter + origin
    place(0, jnp.where(chunk_at > 0, below, 0))
    for near in range(per_chunk):
        start = first_row(first + near) + origin
        for part in range(group_total):
            place(1 + near * group_total + part, start + part * quarter)
    above = first_row(first + per_chunk) + origin
    last = 1 + per_chunk * group_total
    place(last, jnp.where(chunk_at < group_total - 1, above, limit))
    for at in range(0, chunk, LANES):
        out_ref[:, pl.ds(at, LANES)] = rows[pl.ds(pad + at, LANES), :].T.astype(jnp.bfloat16)


def exchange_kernel(
    owners_n, group_total, counts_ref, hidden_any, grad_any, positions_any, quant_any, scales_any,
    grad_out, pieces_out,
    hidden_in, grad_ref, positions_ref, quant_ref, scales_ref,
    weights_ref, rotated, weights, picked, hidden, outgoing, grad_send,
    load_sem, w_send, w_recv, h_send, h_recv,
    up_send, down_send, x_send, y_send, net_recv, pair_send, pair_recv,
    o_send, e_send, o_recv, g_send, g_recv,
):
    here = lax.axis_index("fsdp")
    part = lax.axis_index("tp")
    core = lax.rem(part, 2)
    side = part // 2
    partner = part + 1 - 2 * core
    across = lax.rem(part + 2, group_total)
    tokens, width = grad_ref.shape
    row_total = hidden_in.shape[1]
    quarter = picked.shape[1]
    depth = owners_n // LINE
    z = here // LINE
    y = lax.rem(here, LINE)
    beside = z * LINE + (1 - y)
    per_chunk = owners_n // group_total
    home = here // per_chunk
    last_piece = 1 + per_chunk * group_total

    loads = [pltpu.make_async_copy(grad_any, grad_ref, load_sem.at[0])]
    loads.append(pltpu.make_async_copy(positions_any, positions_ref, load_sem.at[1]))
    columns_each = row_total // LOADS
    for at in range(LOADS):
        columns = pl.ds(at * columns_each, columns_each)
        loads.append(
            pltpu.make_async_copy(hidden_any.at[:, columns], hidden_in.at[:, columns], load_sem.at[4 + at])
        )
    loads.append(pltpu.make_async_copy(quant_any, quant_ref, load_sem.at[2]))
    loads.append(pltpu.make_async_copy(scales_any, scales_ref, load_sem.at[3]))
    for load in loads:
        load.start()
    barrier = pltpu.get_barrier_semaphore()
    for step in range(owners_n):
        for turn in range(group_total):
            if step or turn:
                where = (lax.rem(here + step, owners_n), lax.rem(part + turn, group_total))
                pl.semaphore_signal(barrier, inc=1, device_id=where, device_id_type=MESH)

    def remote(src, dst, send, recv, where):
        return pltpu.make_async_remote_copy(
            src_ref=src, dst_ref=dst, send_sem=send, recv_sem=recv, device_id=where, device_id_type=MESH
        )

    def rows_of(owner):
        return pl.ds(pl.multiple_of(owner * tokens, tokens), tokens)

    def cols_of(group):
        return pl.ds(pl.multiple_of(group * width, width), width)

    def slots_of(group):
        return pl.ds(pl.multiple_of(group * quarter, 16), quarter)

    def weigh(step):
        target = lax.rem(part + step, group_total)
        return remote(
            weights_ref.at[slots_of(target), :], weights.at[:, cols_of(part)],
            w_send.at[step - 1], w_recv.at[step - 1], (here, target),
        )

    def hide(target):
        return remote(
            picked.at[target], hidden.at[:, rows_of(here)],
            h_send.at[target], h_recv.at[here], (target, part),
        )

    def hidden_from(owner):
        return remote(
            picked.at[owner], hidden.at[:, rows_of(owner)],
            h_send.at[owner], h_recv.at[owner], (owner, part),
        )

    def block(owner, row, lane):
        return rotated.at[rows_of(owner), cols_of(2 * row + lane)]

    def relay(owner, row, send, where):
        view = block(owner, row, core)
        return remote(view, view, send, net_recv.at[owner * 2 + row], where)

    def share(owner, row, lane):
        view, at = block(owner, row, lane), owner * 2 + row
        return remote(view, view, pair_send.at[at], pair_recv.at[at], (here, partner))

    offsets = []
    offset = jnp.int32(0)
    for owner in range(owners_n):
        offsets.append(offset)
        offset = offset + counts_ref[owner]

    def pick(owner):
        least, greatest = offset_range(owner, owners_n, row_total, quarter * group_total)
        span = -(-(greatest - least + quarter + LANES) // LANES) * LANES
        base = jnp.minimum((least + part * quarter) // LANES * LANES, row_total - span)
        window = hidden_in[:, pl.ds(pl.multiple_of(base, LANES), span)]
        slot = lax.broadcasted_iota(jnp.int32, (quarter, span), 0)
        column = lax.broadcasted_iota(jnp.int32, (quarter, span), 1)
        first = offsets[owner] + part * quarter - base
        live = jnp.minimum(first + counts_ref[owner] - part * quarter, span)
        chosen = (column == slot + first) & (column < live)
        moved = lax.dot_general(
            chosen.astype(jnp.float32).astype(jnp.bfloat16), window, (((1,), (1,)), ((), ())),
            preferred_element_type=jnp.float32,
        )
        picked[owner] = moved.astype(jnp.bfloat16)

    loads[0].wait()
    loads[1].wait()
    heads = scales_ref.shape[0]
    lane = lax.broadcasted_iota(jnp.int32, (tokens, HD), 1)
    pair_at = jnp.where(lane < HD // 2, lane, lane - HD // 2).astype(jnp.float32)
    inverse = jnp.exp(-(2.0 * pair_at / HD) * math.log(rope_base))
    place = jnp.broadcast_to(positions_ref[...].astype(jnp.float32), (HD, tokens)).T
    angles = place * inverse
    cosine = jnp.cos(angles)
    sine = jnp.sin(angles)
    sine = jnp.where(lane < HD // 2, sine, -sine)
    for head in range(heads):
        values = grad_ref[:, pl.ds(head * HD, HD)].astype(jnp.float32)
        swapped = jnp.concatenate([values[:, HD // 2 :], values[:, : HD // 2]], axis=1)
        cols = pl.ds(pl.multiple_of(part * width + head * HD, HD), HD)
        rotated[rows_of(here), cols] = (values * cosine + swapped * sine).astype(jnp.bfloat16)
    for load in loads[2 : 2 + LOADS]:
        load.wait()
    order = []
    for low in range((depth + 1) // 2):
        for level in dict.fromkeys((depth - 1 - low, low)):
            order += [level * LINE + row for row in range(LINE)]
    for owner in order[: 2 * LINE]:
        pick(owner)
    with jax.named_scope("barrier"):
        pl.semaphore_wait(barrier, owners_n * group_total - 1)

    def begin(copy):
        copy.start()

    def finish(copy):
        copy.wait_send()

    def from_z(level, up, down, act):
        owner = level * LINE + y

        @pl.when(up)
        def _():
            act(relay(owner, side, up_send.at[owner], (here + LINE, part)))

        @pl.when(down)
        def _():
            act(relay(owner, side, down_send.at[owner], (here - LINE, part)))

        act(relay(owner, side, x_send.at[owner], (here, across)))
        act(relay(owner, side, y_send.at[owner * 2 + side], (beside, part)))
        act(share(owner, side, core))

    def from_x(level, act):
        owner = level * LINE + y
        act(relay(owner, 1 - side, y_send.at[owner * 2 + 1 - side], (beside, part)))
        act(share(owner, 1 - side, core))

    def from_y(level, row, act):
        act(share(level * LINE + 1 - y, row, core))

    def arrived(owner, row):
        relay(owner, row, x_send.at[0], (here, across)).wait_recv()

    def levels(away):
        for sign in (-1, 1) if away else (1,):
            yield sign, z + sign * away

    def at_levels(away, act):
        if 0 <= away < depth:
            for sign, level in levels(away):

                @pl.when((level >= 0) & (level < depth))
                def _():
                    act(sign, level)

    def hide_item(item):
        level, row = item // LINE, (1 - y if item % LINE == 0 else y)
        above = depth - 1 - level

        @pl.when(above > z)
        def _():
            hide(above * LINE + row).start()

        @pl.when(level < z)
        def _():
            hide(level * LINE + row).start()

    from_z(z, z < depth - 1, z > 0, begin)
    hide_item(0)
    for load in loads[2 + LOADS :]:
        load.wait()
    for head in range(heads):
        cols = pl.ds(head * HD, HD)
        scale = jnp.broadcast_to(scales_ref[head : head + 1, :], (HD, scales_ref.shape[1])).T
        weights_ref[:, cols] = (quant_ref[:, cols].astype(jnp.float32) * scale).astype(jnp.bfloat16)
    for owner in order[2 * LINE :]:
        pick(owner)
    hide(beside).start()
    for step in range(1, group_total):
        weigh(step).start()
    weights[:, cols_of(part)] = weights_ref[slots_of(part), :]
    hidden[:, rows_of(here)] = picked[here]

    def send_piece(owner, act):
        source = outgoing.at[owner]
        index = 1 + lax.rem(here, per_chunk) * group_total + part
        mine = (owner == here) & (home == part)

        @pl.when(jnp.logical_not(mine))
        def _():
            act(remote(source, pieces_out.at[index], o_send.at[owner], o_recv.at[index], (owner, home)))

        if act is begin:

            @pl.when(mine)
            def _():
                pieces_out[index] = outgoing[owner]

    def produce(owner):
        with jax.named_scope("shared"):
            for row in range(2):
                share(owner, row, 1 - core).wait_recv()
        outgoing[owner] = lax.dot_general(
            weights[...], rotated[rows_of(owner), :], (((1,), (1,)), ((), ())),
            preferred_element_type=jnp.float32,
        ).astype(jnp.bfloat16)

    hidden_items = LINE * (depth - 1)
    sent = 1
    for stage in range(1, depth + 3):

        def take_z(sign, level):
            with jax.named_scope(f"z{stage}{sign}"):
                arrived(level * LINE + y, side)
            from_z(level, (sign < 0) & (z < depth - 1), (sign > 0) & (z > 0), begin)

        def take_x(sign, level):
            with jax.named_scope(f"x{stage}{sign}"):
                arrived(level * LINE + y, 1 - side)
            from_x(level, begin)

        def take_y(row):
            def act(sign, level):
                with jax.named_scope(f"y{stage}{sign}"):
                    arrived(level * LINE + 1 - y, row)
                from_y(level, row, begin)

            return act

        if stage < depth:
            at_levels(stage, take_z)
        at_levels(stage - 1, take_x)
        at_levels(stage - 1, take_y(side))
        at_levels(stage - 2, take_y(1 - side))
        for item in range(sent, min(sent + HIDE_EACH, hidden_items)):
            hide_item(item)
        sent = min(sent + HIDE_EACH, hidden_items)
        if stage == 1:
            with jax.named_scope("weigh"):
                for step in range(1, group_total):
                    weigh(step).wait_recv()
        at_levels(stage - 1, lambda sign, level: produce(level * LINE + y))
        at_levels(stage - 2, lambda sign, level: produce(level * LINE + 1 - y))
        at_levels(stage - 1, lambda sign, level: send_piece(level * LINE + y, begin))
        at_levels(stage - 2, lambda sign, level: send_piece(level * LINE + 1 - y, begin))

    with jax.named_scope("hidden"):
        for step in range(1, owners_n):
            hidden_from(lax.rem(here + step, owners_n)).wait_recv()

    def send_grad(step):
        target = lax.rem(part + step, group_total)
        return remote(
            grad_send.at[target], grad_out.at[part], g_send.at[step - 1], g_recv.at[step - 1], (here, target)
        )

    def reduce(step, carry):
        target = lax.rem(part + step, group_total)
        grad_send[target] = jnp.dot(
            hidden[...], rotated[:, cols_of(target)], preferred_element_type=jnp.float32
        ).astype(jnp.bfloat16)

        @pl.when(step > 1)
        def _():
            send_grad(step - 1).start()

        return carry

    with jax.named_scope("reduce"):
        lax.fori_loop(1, group_total + 1, reduce, 0)
    grad_out[part] = grad_send[part]

    mine_index = jnp.where(home == part, 1 + lax.rem(here, per_chunk) * group_total + part, 0)

    def landed(index):
        return remote(
            outgoing.at[0], pieces_out.at[index], o_send.at[0], o_recv.at[index], (here, partner)
        )

    def pass_on(index, to_chunk, slot, send):
        return remote(pieces_out.at[index], pieces_out.at[slot], e_send.at[send], o_recv.at[slot], (here, to_chunk))

    for index in (last_piece - 1, 1):

        @pl.when(mine_index != index)
        def _():
            with jax.named_scope("edge"):
                landed(index).wait_recv()

    @pl.when(part < group_total - 1)
    def _():
        pass_on(last_piece - 1, part + 1, 0, 0).start()

    @pl.when(part > 0)
    def _():
        pass_on(1, part - 1, last_piece, 1).start()

    for index in range(2, last_piece - 1):

        @pl.when(mine_index != index)
        def _():
            with jax.named_scope("landed"):
                landed(index).wait_recv()

    @pl.when(part < group_total - 1)
    def _():
        pass_on(last_piece - 1, part + 1, 0, 0).wait_send()
        landed(last_piece).wait_recv()

    @pl.when(part > 0)
    def _():
        pass_on(1, part - 1, last_piece, 1).wait_send()
        landed(0).wait_recv()

    with jax.named_scope("grads"):
        for step in range(1, group_total):
            send_grad(step).wait_send()
            remote(grad_send.at[0], grad_out.at[0], g_send.at[step - 1], g_recv.at[step - 1], (here, partner)).wait_recv()
    for owner in range(owners_n):
        send_piece(jnp.int32(owner), finish)
    for step in range(1, group_total):
        weigh(step).wait_send()
    for step in range(1, owners_n):
        hide(lax.rem(here + step, owners_n)).wait_send()
    from_z(z, z < depth - 1, z > 0, finish)
    for away in range(depth):
        if away:
            at_levels(
                away,
                lambda sign, level: from_z(level, (sign < 0) & (z < depth - 1), (sign > 0) & (z > 0), finish),
            )
        at_levels(away, lambda sign, level: from_x(level, finish))
        for row in range(2):
            at_levels(away, lambda sign, level, row=row: from_y(level, row, finish))


def exchange_plan(hidden_in, key_grad, positions, key_quant, key_scales, block_counts):
    owners_n = lax.axis_size("fsdp")
    group_total = lax.axis_size("tp")
    slot_count, width = key_quant.shape
    tokens_here, row_total = hidden_in.shape
    heads = key_scales.shape[1]
    quarter = slot_count // group_total
    chunk = row_total // group_total
    per_chunk = owners_n // group_total
    columns = width * group_total
    vmem = pl.BlockSpec(memory_space=pltpu.VMEM)
    anywhere = pl.BlockSpec(memory_space=pl.ANY)
    smem = pl.BlockSpec(memory_space=pltpu.SMEM)
    pieces_n = 2 + per_chunk * group_total
    dma = pltpu.SemaphoreType.DMA
    weight_grad, pieces = pl.pallas_call(
        functools.partial(exchange_kernel, owners_n, group_total),
        out_shape=(
            jax.ShapeDtypeStruct((group_total, quarter, width), jnp.bfloat16),
            jax.ShapeDtypeStruct((pieces_n, quarter, tokens_here), jnp.bfloat16),
        ),
        in_specs=[smem] + [anywhere] * 5,
        out_specs=(vmem,) * 2,
        scratch_shapes=[
            pltpu.VMEM((tokens_here, row_total), jnp.bfloat16),
            pltpu.VMEM((tokens_here, width), jnp.bfloat16),
            pltpu.VMEM((1, tokens_here), jnp.int32),
            pltpu.VMEM((slot_count, width), jnp.bfloat16),
            pltpu.VMEM((heads, slot_count), jnp.float32),
            pltpu.VMEM((slot_count, width), jnp.bfloat16),
            pltpu.VMEM((owners_n * tokens_here, columns), jnp.bfloat16),
            pltpu.VMEM((quarter, columns), jnp.bfloat16),
            pltpu.VMEM((owners_n, quarter, tokens_here), jnp.bfloat16),
            pltpu.VMEM((quarter, owners_n * tokens_here), jnp.bfloat16),
            pltpu.VMEM((owners_n, quarter, tokens_here), jnp.bfloat16),
            pltpu.VMEM((group_total, quarter, width), jnp.bfloat16),
            dma((4 + LOADS,)),
            dma((group_total - 1,)), dma((group_total - 1,)),
            dma((owners_n,)), dma((owners_n,)),
            dma((owners_n,)), dma((owners_n,)), dma((owners_n,)), dma((2 * owners_n,)), dma((2 * owners_n,)),
            dma((2 * owners_n,)), dma((2 * owners_n,)),
            dma((owners_n,)), dma((2,)), dma((pieces_n,)),
            dma((group_total - 1,)), dma((group_total - 1,)),
        ],
        compiler_params=pltpu.CompilerParams(has_side_effects=True, collective_id=0),
        name="exchange",
    )(block_counts, hidden_in, key_grad, positions.reshape(1, -1), key_quant, key_scales.T)

    margin = max(
        max(
            chunk * (owner // per_chunk) - offset_range(owner - 1, owners_n, row_total, slot_count)[0]
            for owner in range(per_chunk, owners_n, per_chunk)
        ),
        2 * quarter,
    ) if group_total > 1 else 2 * quarter
    pad = -(-(margin + slot_count) // 8) * 8
    return pl.pallas_call(
        functools.partial(assemble_kernel, owners_n, group_total, pad),
        out_shape=(
            jax.ShapeDtypeStruct((slot_count, width), jnp.bfloat16),
            jax.ShapeDtypeStruct((tokens_here, chunk), jnp.bfloat16),
        ),
        in_specs=[smem, vmem, vmem],
        out_specs=(vmem,) * 2,
        scratch_shapes=[pltpu.VMEM((chunk + 2 * pad, tokens_here), jnp.float32)],
        name="assemble",
    )(block_counts, pieces, weight_grad)


def rotary_backward(key_grad, positions):
    tokens_here = key_grad.shape[0]
    half_dim = HD // 2
    cotangent = key_grad.astype(jnp.float32).reshape(tokens_here, -1, HD)
    freq_idx = jnp.arange(half_dim, dtype=jnp.float32)
    inverse = jnp.exp(-(2.0 * freq_idx / HD) * math.log(rope_base))
    angles = positions.astype(jnp.float32)[:, None] * inverse[None, :]
    cosine = jnp.cos(angles)[:, None, :]
    sine_part = jnp.sin(angles)[:, None, :]
    lower_half = cotangent[..., :half_dim]
    upper_half = cotangent[..., half_dim:]
    back_lower = lower_half * cosine + upper_half * sine_part
    back_upper = upper_half * cosine - lower_half * sine_part
    joined = jnp.concatenate([back_lower, back_upper], axis=-1)
    return joined.reshape(tokens_here, -1).astype(jnp.bfloat16)


def slot_tables(block_counts, slot_count, row_total):
    offsets = jnp.cumsum(block_counts) - block_counts
    owners_n = block_counts.shape[0]
    slot_ids = jnp.arange(owners_n * slot_count, dtype=jnp.int32)
    within = slot_ids % slot_count
    live_counts = jnp.broadcast_to(block_counts[:, None], (owners_n, slot_count)).reshape(-1)
    base_rows = jnp.broadcast_to(offsets[:, None], (owners_n, slot_count)).reshape(-1)
    is_live = within < live_counts
    row_of_slot = jnp.where(is_live, base_rows + within, 0)
    row_ids = jnp.arange(row_total, dtype=jnp.int32)
    at_or_after = row_ids[:, None] >= offsets[None, :]
    owner_of_row = jnp.sum(at_or_after.astype(jnp.int32), axis=1) - 1
    row_begin = jnp.max(jnp.where(at_or_after, offsets[None, :], 0), axis=1)
    slot_of_row = owner_of_row * slot_count + row_ids - row_begin
    return (row_of_slot, is_live, slot_of_row)


def gather_plan(hidden_in, key_grad, positions, key_quant, key_scales, block_counts):
    slot_count = key_quant.shape[0]
    local_heads = key_scales.shape[1]
    row_total = hidden_in.shape[1]
    row_of_slot, is_live, slot_of_row = slot_tables(block_counts, slot_count, row_total)
    scaled = (
        key_quant.astype(jnp.float32).reshape(slot_count, local_heads, HD) * key_scales[:, :, None]
    )
    local_weights = scaled.astype(jnp.bfloat16).reshape(slot_count, local_heads * HD)
    rotated = rotary_backward(key_grad, positions)
    picked = jnp.where(
        is_live[None, :], jnp.take(hidden_in, row_of_slot, axis=1), jnp.zeros((), jnp.bfloat16)
    )
    weight_grad = lax.psum_scatter(
        lax.dot_general(
            picked, rotated, (((0,), (0,)), ((), ())), preferred_element_type=jnp.float32
        ),
        "fsdp",
        scatter_dimension=0,
        tiled=True,
    ).astype(jnp.bfloat16)
    group_total = lax.axis_size("tp")
    whole_slots = lax.all_gather(local_weights, "fsdp", axis=0, tiled=True)
    ordered = jnp.take(whole_slots, slot_of_row, axis=0)
    own_rows = lax.all_to_all(ordered, "tp", split_axis=0, concat_axis=1, tiled=True)
    all_heads = lax.all_gather(rotated, "tp", axis=1, tiled=True)
    tokens_here = all_heads.shape[0]
    feature_here = own_rows.shape[0]
    heads_grouped = all_heads.reshape(tokens_here, group_total, -1)
    rows_grouped = own_rows.reshape(feature_here, group_total, -1)
    group_part = jnp.einsum(
        "tgk,dgk->gtd", heads_grouped, rows_grouped, preferred_element_type=jnp.float32
    ).astype(jnp.bfloat16)
    input_grad = jnp.sum(group_part.astype(jnp.float32), axis=0).astype(jnp.bfloat16)
    return (weight_grad, input_grad)


def per_device(hidden_in, key_grad, positions, key_quant, key_scales, block_counts):
    tokens_here, row_total = hidden_in.shape
    slot_count, width = key_quant.shape
    fits = exchange_fits(
        lax.axis_size("fsdp"), lax.axis_size("tp"), slot_count, row_total, tokens_here, width
    )
    plan = exchange_plan if fits else gather_plan
    return plan(hidden_in, key_grad, positions, key_quant, key_scales, block_counts)


def solution(mesh):
    in_specs = (P("fsdp", None), P("fsdp", "tp"), P("fsdp"), P("fsdp", "tp"), P("fsdp", "tp"), P())
    out_specs = (P("fsdp", "tp"), P("fsdp", "tp"))
    return jax.shard_map(
        per_device, mesh=mesh, in_specs=in_specs, out_specs=out_specs, check_vma=False
    )
```

```python
import functools
import math

import jax
import jax.numpy as jnp
from jax import lax
from jax.experimental import pallas as pl
from jax.experimental.pallas import tpu as pltpu
from jax.sharding import PartitionSpec as P

HD = 128
LANES = 128
LINE = 2
LOADS = 4
VMEM_LIMIT = 24 * 2**20
WEIGH_AT = 4
WEIGH_NEXT = 1
OUT_AT = 4
MESH = pl.DeviceIdType.MESH

rope_base = 500000.0


def offset_range(index, owners_n, row_total, slot_count):
    least_count = 2 * row_total // owners_n - slot_count
    later = owners_n - index
    least = max(index * least_count, row_total - later * slot_count)
    greatest = min(index * slot_count, row_total - later * least_count)
    return least, greatest


def exchange_fits(owners_n, group_total, slot_count, row_total, tokens_here, width):
    if group_total != 2 * LINE or owners_n % group_total or owners_n % LINE or slot_count % (16 * group_total):
        return False
    if tokens_here % LANES or width % LANES or row_total % group_total or (row_total // group_total) % LANES:
        return False
    quarter = slot_count // group_total
    chunk = row_total // group_total
    per_chunk = owners_n // group_total
    if 2 * row_total // owners_n - slot_count < quarter or row_total < 2 * quarter + 4 * LANES:
        return False
    for owner in range(owners_n):
        least, greatest = offset_range(owner, owners_n, row_total, slot_count)
        home = owner // per_chunk
        if greatest - least + quarter + 2 * LANES > row_total:
            return False
        for part in range(group_total):
            reach = range(
                max(0, (least + part * quarter) // chunk),
                min(group_total - 1, (greatest + (part + 1) * quarter - 1) // chunk) + 1,
            )
            allowed = {home}
            if part == 0 and owner % per_chunk == 0:
                allowed.add(home - 1)
            if part == group_total - 1 and owner % per_chunk == per_chunk - 1:
                allowed.add(home + 1)
            if not set(reach) <= allowed:
                return False
    return True


def assemble_kernel(owners_n, group_total, pad, counts_ref, pieces_ref, grad_ref, grad_out, out_ref, rows):
    chunk_at = lax.axis_index("tp")
    chunk = out_ref.shape[1]
    quarter = pieces_ref.shape[1]
    per_chunk = owners_n // group_total
    offsets = []
    offset = jnp.int32(0)
    for owner in range(owners_n):
        offsets.append(offset)
        offset = offset + counts_ref[owner]

    def first_row(owner):
        found = jnp.int32(0)
        for candidate in range(owners_n):
            found = jnp.where(owner == candidate, offsets[candidate], found)
        return found

    limit = rows.shape[0] - quarter

    def place(index, begin):
        rows[pl.ds(jnp.clip(begin, 0, limit), quarter), :] = pieces_ref[index].astype(jnp.float32)

    for part in range(group_total):
        grad_out[pl.ds(part * quarter, quarter), :] = grad_ref[part]
    origin = pad - chunk_at * chunk
    first = chunk_at * per_chunk
    below = first_row(first - 1) + (group_total - 1) * quarter + origin
    place(0, jnp.where(chunk_at > 0, below, 0))
    for near in range(per_chunk):
        start = first_row(first + near) + origin
        for part in range(group_total):
            place(1 + near * group_total + part, start + part * quarter)
    above = first_row(first + per_chunk) + origin
    last = 1 + per_chunk * group_total
    place(last, jnp.where(chunk_at < group_total - 1, above, limit))
    for at in range(0, chunk, LANES):
        out_ref[:, pl.ds(at, LANES)] = rows[pl.ds(pad + at, LANES), :].T.astype(jnp.bfloat16)


def exchange_kernel(
    owners_n, group_total, counts_ref, hidden_any, grad_any, positions_any, quant_any, scales_any,
    grad_out, pieces_out,
    hidden_in, grad_ref, positions_ref, quant_ref, scales_ref,
    weights_ref, rotated, weights, picked, hidden, outgoing, grad_send,
    load_sem, w_send, w_recv, h_send, h_recv,
    z_send, first_send, second_send, net_recv, pair_send, pair_recv,
    o_send, e_send, o_recv, g_send, g_recv,
    column_in, beside_in,
):
    here = lax.axis_index("fsdp")
    part = lax.axis_index("tp")
    core = lax.rem(part, 2)
    side = part // 2
    partner = part + 1 - 2 * core
    across = lax.rem(part + 2, group_total)
    tokens, width = grad_ref.shape
    row_total = hidden_in.shape[1]
    quarter = picked.shape[1]
    depth = owners_n // LINE
    z = here // LINE
    y = lax.rem(here, LINE)
    beside = z * LINE + (1 - y)
    per_chunk = owners_n // group_total
    home = here // per_chunk
    last_piece = 1 + per_chunk * group_total

    loads = [pltpu.make_async_copy(grad_any, grad_ref, load_sem.at[0])]
    loads.append(pltpu.make_async_copy(positions_any, positions_ref, load_sem.at[1]))
    columns_each = row_total // LOADS
    for at in range(LOADS):
        columns = pl.ds(at * columns_each, columns_each)
        loads.append(
            pltpu.make_async_copy(hidden_any.at[:, columns], hidden_in.at[:, columns], load_sem.at[4 + at])
        )
    loads.append(pltpu.make_async_copy(quant_any, quant_ref, load_sem.at[2]))
    loads.append(pltpu.make_async_copy(scales_any, scales_ref, load_sem.at[3]))
    for load in loads:
        load.start()
    barrier = pltpu.get_barrier_semaphore()

    def greet(where):
        pl.semaphore_signal(barrier, inc=1, device_id=where, device_id_type=MESH)

    @pl.when(z > 0)
    def _():
        greet((here - LINE, part))

    @pl.when(z < depth - 1)
    def _():
        greet((here + LINE, part))

    for row in range(LINE):
        for turn in range(group_total):
            if row or turn:
                greet((z * LINE + lax.rem(y + row, LINE), lax.rem(part + turn, group_total)))
    near_n = LINE * group_total - 1 + jnp.where(z > 0, 1, 0) + jnp.where(z < depth - 1, 1, 0)

    def remote(src, dst, send, recv, where):
        return pltpu.make_async_remote_copy(
            src_ref=src, dst_ref=dst, send_sem=send, recv_sem=recv, device_id=where, device_id_type=MESH
        )

    def rows_of(owner):
        return pl.ds(pl.multiple_of(owner * tokens, tokens), tokens)

    def cols_of(group):
        return pl.ds(pl.multiple_of(group * width, width), width)

    def slots_of(group):
        return pl.ds(pl.multiple_of(group * quarter, 16), quarter)

    peers = (lax.rem(partner + 2, group_total), across, partner)

    def weigh(kind):
        return remote(
            weights_ref.at[slots_of(peers[kind]), :], weights.at[:, cols_of(part)],
            w_send.at[kind], w_recv.at[kind], (here, peers[kind]),
        )

    def hide(target):
        return remote(
            picked.at[target], hidden.at[:, rows_of(here)],
            h_send.at[target], h_recv.at[here], (target, part),
        )

    def hidden_from(owner):
        return remote(
            picked.at[owner], hidden.at[:, rows_of(owner)],
            h_send.at[owner], h_recv.at[owner], (owner, part),
        )

    def block(owner, row, lane):
        return rotated.at[rows_of(owner), cols_of(2 * row + lane)]

    def relay(owner, row, send, where):
        view = block(owner, row, core)
        return remote(view, view, send, net_recv.at[owner * 2 + row], where)

    def share(owner, row, lane):
        view, at = block(owner, row, lane), owner * 2 + row
        return remote(view, view, pair_send.at[at], pair_recv.at[at], (here, partner))

    offsets = []
    offset = jnp.int32(0)
    for owner in range(owners_n):
        offsets.append(offset)
        offset = offset + counts_ref[owner]

    def pick(owner):
        least, greatest = offset_range(owner, owners_n, row_total, quarter * group_total)
        span = -(-(greatest - least + quarter + LANES) // LANES) * LANES
        base = jnp.minimum((least + part * quarter) // LANES * LANES, row_total - span)
        window = hidden_in[:, pl.ds(pl.multiple_of(base, LANES), span)]
        slot = lax.broadcasted_iota(jnp.int32, (quarter, span), 0)
        column = lax.broadcasted_iota(jnp.int32, (quarter, span), 1)
        first = offsets[owner] + part * quarter - base
        live = jnp.minimum(first + counts_ref[owner] - part * quarter, span)
        chosen = (column == slot + first) & (column < live)
        moved = lax.dot_general(
            chosen.astype(jnp.float32).astype(jnp.bfloat16), window, (((1,), (1,)), ((), ())),
            preferred_element_type=jnp.float32,
        )
        picked[owner] = moved.astype(jnp.bfloat16)

    loads[0].wait()
    loads[1].wait()
    heads = scales_ref.shape[0]
    lane = lax.broadcasted_iota(jnp.int32, (tokens, HD), 1)
    pair_at = jnp.where(lane < HD // 2, lane, lane - HD // 2).astype(jnp.float32)
    inverse = jnp.exp(-(2.0 * pair_at / HD) * math.log(rope_base))
    place = jnp.broadcast_to(positions_ref[...].astype(jnp.float32), (HD, tokens)).T
    angles = place * inverse
    cosine = jnp.cos(angles)
    sine = jnp.sin(angles)
    sine = jnp.where(lane < HD // 2, sine, -sine)
    for head in range(heads):
        values = grad_ref[:, pl.ds(head * HD, HD)].astype(jnp.float32)
        swapped = jnp.concatenate([values[:, HD // 2 :], values[:, : HD // 2]], axis=1)
        cols = pl.ds(pl.multiple_of(part * width + head * HD, HD), HD)
        rotated[rows_of(here), cols] = (values * cosine + swapped * sine).astype(jnp.bfloat16)
    with jax.named_scope("barrier"):
        pl.semaphore_wait(barrier, near_n)

    def begin(copy):
        copy.start()

    def finish(copy):
        copy.wait_send()

    def own_row(level):
        return level * LINE + y, side

    def first_row(level):
        return level * LINE + jnp.where(core == 0, y, 1 - y), jnp.where(core == 0, 1 - side, side)

    def second_row(level):
        return level * LINE + jnp.where(core == 0, 1 - y, y), jnp.where(core == 0, side, 1 - side)

    def last_row(level):
        return level * LINE + 1 - y, 1 - side

    first_to = (jnp.where(core == 0, here, beside), jnp.where(core == 0, across, part))
    second_to = (jnp.where(core == 0, beside, here), jnp.where(core == 0, part, across))

    def climb(level):
        return relay(*own_row(z), z_send.at[level], (level * LINE + y, part))

    def from_z(level, act):
        owner, row = own_row(level)
        act(relay(owner, row, first_send.at[owner], first_to))
        act(relay(owner, row, second_send.at[owner * 2 + row], second_to))
        act(share(owner, row, core))

    def from_first(level, act):
        owner, row = first_row(level)
        act(relay(owner, row, second_send.at[owner * 2 + row], second_to))
        act(share(owner, row, core))

    def from_second(level, act):
        act(share(*second_row(level), core))

    def from_last(level, act):
        act(share(*last_row(level), core))

    def arrived(owner, row):
        relay(owner, row, first_send.at[0], first_to).wait_recv()

    def levels(away):
        for sign in (-1, 1) if away else (1,):
            yield sign, z + sign * away

    def at_levels(away, act):
        if 0 <= away < depth:
            for sign, level in levels(away):

                @pl.when((level >= 0) & (level < depth))
                def _():
                    act(sign, level)

    def tell(level, known):
        pl.semaphore_signal(
            column_in.at[known], inc=1, device_id=(level * LINE + y, part), device_id_type=MESH
        )

    def heard(sign, known):
        @pl.when((z - sign >= 0) & (z - sign < depth))
        def _():
            tell(z - sign, known)

    at_levels(1, heard)
    at_levels(1, lambda sign, level: climb(level).start())
    from_z(z, begin)

    def farther(sign, level):
        pl.semaphore_wait(column_in.at[level], 1)
        heard(sign, level)
        climb(level).start()

    for away in range(2, depth):
        at_levels(away, farther)
    pl.semaphore_signal(beside_in, inc=1, device_id=(beside, part), device_id_type=MESH)
    for load in loads[2 : 2 + LOADS]:
        load.wait()
    for owner in range(owners_n):
        pick(owner)
    for load in loads[2 + LOADS :]:
        load.wait()
    for head in range(heads):
        cols = pl.ds(head * HD, HD)
        scale = jnp.broadcast_to(scales_ref[head : head + 1, :], (HD, scales_ref.shape[1])).T
        weights_ref[:, cols] = (quant_ref[:, cols].astype(jnp.float32) * scale).astype(jnp.bfloat16)
    weights[:, cols_of(part)] = weights_ref[slots_of(part), :]
    hidden[:, rows_of(here)] = picked[here]
    weigh(1).start()
    weigh(2).start()
    pl.semaphore_wait(beside_in, 1)
    for row in (1 - y, y):
        for away in range(1, depth):
            at_levels(away, lambda sign, level, row=row: hide(level * LINE + row).start())
    hide(beside).start()

    def send_piece(owner, act):
        source = outgoing.at[owner]
        index = 1 + lax.rem(here, per_chunk) * group_total + part
        mine = (owner == here) & (home == part)

        @pl.when(jnp.logical_not(mine))
        def _():
            act(remote(source, pieces_out.at[index], o_send.at[owner], o_recv.at[index], (owner, home)))

        if act is begin:

            @pl.when(mine)
            def _():
                pieces_out[index] = outgoing[owner]

    def produce(owner):
        with jax.named_scope("shared"):
            for row in range(2):
                share(owner, row, 1 - core).wait_recv()
        outgoing[owner] = lax.dot_general(
            weights[...], rotated[rows_of(owner), :], (((1,), (1,)), ((), ())),
            preferred_element_type=jnp.float32,
        ).astype(jnp.bfloat16)

    ready, made = [], []
    for stage in range(1, depth + 3):

        def take(name, row_of, pass_on):
            def act(sign, level):
                with jax.named_scope(f"{name}{stage}{sign}"):
                    arrived(*row_of(level))
                pass_on(sign, level)

            return act

        if stage < depth:
            at_levels(stage, take("z", own_row, lambda sign, level: from_z(level, begin)))
        at_levels(stage - 1, take("first", first_row, lambda sign, level: from_first(level, begin)))
        at_levels(stage - 1, take("second", second_row, lambda sign, level: from_second(level, begin)))
        at_levels(stage - 2, take("last", last_row, lambda sign, level: from_last(level, begin)))
        if stage == WEIGH_NEXT:
            weigh(0).start()
        if stage == WEIGH_AT:
            with jax.named_scope("weigh"):
                for kind in range(3):
                    weigh(kind).wait_recv()
        ready.append((stage - 1, y))
        ready.append((stage - 2, 1 - y))
        if stage >= WEIGH_AT:
            for away, row in ready:
                at_levels(away, lambda sign, level, row=row: produce(level * LINE + row))
            made += ready
            ready = []
        if stage >= OUT_AT:
            for away, row in made[::-1]:
                at_levels(away, lambda sign, level, row=row: send_piece(level * LINE + row, begin))
            made = []

    with jax.named_scope("hidden"):
        for step in range(1, owners_n):
            hidden_from(lax.rem(here + step, owners_n)).wait_recv()

    def send_grad(kind):
        return remote(
            grad_send.at[peers[kind]], grad_out.at[part], g_send.at[kind], g_recv.at[kind], (here, peers[kind])
        )

    with jax.named_scope("reduce"):
        for kind, target in enumerate(peers + (part,)):
            grad_send[target] = jnp.dot(
                hidden[...], rotated[:, cols_of(target)], preferred_element_type=jnp.float32
            ).astype(jnp.bfloat16)
            if kind:
                send_grad(kind - 1).start()
    grad_out[part] = grad_send[part]

    for kind in range(3):
        weigh(kind).wait_send()
    for step in range(1, owners_n):
        hide(lax.rem(here + step, owners_n)).wait_send()
    for away in range(depth):
        if away:
            at_levels(away, lambda sign, level: climb(level).wait_send())
        at_levels(away, lambda sign, level: from_z(level, finish))
        at_levels(away, lambda sign, level: from_first(level, finish))
        at_levels(away, lambda sign, level: from_second(level, finish))
        at_levels(away, lambda sign, level: from_last(level, finish))

    mine_index = jnp.where(home == part, 1 + lax.rem(here, per_chunk) * group_total + part, 0)

    def landed(index):
        return remote(
            outgoing.at[0], pieces_out.at[index], o_send.at[0], o_recv.at[index], (here, partner)
        )

    def pass_on(index, to_chunk, slot, send):
        return remote(pieces_out.at[index], pieces_out.at[slot], e_send.at[send], o_recv.at[slot], (here, to_chunk))

    for index in (last_piece - 1, 1):

        @pl.when(mine_index != index)
        def _():
            with jax.named_scope("edge"):
                landed(index).wait_recv()

    @pl.when(part < group_total - 1)
    def _():
        pass_on(last_piece - 1, part + 1, 0, 0).start()

    @pl.when(part > 0)
    def _():
        pass_on(1, part - 1, last_piece, 1).start()

    for index in range(2, last_piece - 1):

        @pl.when(mine_index != index)
        def _():
            with jax.named_scope("landed"):
                landed(index).wait_recv()

    @pl.when(part < group_total - 1)
    def _():
        pass_on(last_piece - 1, part + 1, 0, 0).wait_send()
        landed(last_piece).wait_recv()

    @pl.when(part > 0)
    def _():
        pass_on(1, part - 1, last_piece, 1).wait_send()
        landed(0).wait_recv()

    for owner in range(owners_n):
        send_piece(jnp.int32(owner), finish)
    with jax.named_scope("grads"):
        for kind in range(3):
            send_grad(kind).wait_send()
            remote(grad_send.at[0], grad_out.at[0], g_send.at[kind], g_recv.at[kind], (here, partner)).wait_recv()


def exchange_plan(hidden_in, key_grad, positions, key_quant, key_scales, block_counts):
    owners_n = lax.axis_size("fsdp")
    group_total = lax.axis_size("tp")
    slot_count, width = key_quant.shape
    tokens_here, row_total = hidden_in.shape
    heads = key_scales.shape[1]
    quarter = slot_count // group_total
    chunk = row_total // group_total
    per_chunk = owners_n // group_total
    columns = width * group_total
    vmem = pl.BlockSpec(memory_space=pltpu.VMEM)
    anywhere = pl.BlockSpec(memory_space=pltpu.HBM)
    smem = pl.BlockSpec(memory_space=pltpu.SMEM)
    pieces_n = 2 + per_chunk * group_total
    dma = pltpu.SemaphoreType.DMA
    weight_grad, pieces = pl.pallas_call(
        functools.partial(exchange_kernel, owners_n, group_total),
        out_shape=(
            jax.ShapeDtypeStruct((group_total, quarter, width), jnp.bfloat16),
            jax.ShapeDtypeStruct((pieces_n, quarter, tokens_here), jnp.bfloat16),
        ),
        in_specs=[smem] + [anywhere] * 5,
        out_specs=(vmem,) * 2,
        scratch_shapes=[
            pltpu.VMEM((tokens_here, row_total), jnp.bfloat16),
            pltpu.VMEM((tokens_here, width), jnp.bfloat16),
            pltpu.VMEM((1, tokens_here), jnp.int32),
            pltpu.VMEM((slot_count, width), jnp.bfloat16),
            pltpu.VMEM((heads, slot_count), jnp.float32),
            pltpu.VMEM((slot_count, width), jnp.bfloat16),
            pltpu.VMEM((owners_n * tokens_here, columns), jnp.bfloat16),
            pltpu.VMEM((quarter, columns), jnp.bfloat16),
            pltpu.VMEM((owners_n, quarter, tokens_here), jnp.bfloat16),
            pltpu.VMEM((quarter, owners_n * tokens_here), jnp.bfloat16),
            pltpu.VMEM((owners_n, quarter, tokens_here), jnp.bfloat16),
            pltpu.VMEM((group_total, quarter, width), jnp.bfloat16),
            dma((4 + LOADS,)),
            dma((group_total - 1,)), dma((group_total - 1,)),
            dma((owners_n,)), dma((owners_n,)),
            dma((owners_n // LINE,)), dma((owners_n,)), dma((2 * owners_n,)), dma((2 * owners_n,)),
            dma((2 * owners_n,)), dma((2 * owners_n,)),
            dma((owners_n,)), dma((2,)), dma((pieces_n,)),
            dma((group_total - 1,)), dma((group_total - 1,)),
            pltpu.SemaphoreType.REGULAR((owners_n // LINE,)), pltpu.SemaphoreType.REGULAR,
        ],
        compiler_params=pltpu.CompilerParams(
            has_side_effects=True, collective_id=0, vmem_limit_bytes=VMEM_LIMIT
        ),
        name="exchange",
    )(*(
        pltpu.with_memory_space_constraint(array, pltpu.HBM)
        for array in (block_counts, hidden_in, key_grad, positions.reshape(1, -1), key_quant, key_scales.T)
    ))

    margin = max(
        max(
            chunk * (owner // per_chunk) - offset_range(owner - 1, owners_n, row_total, slot_count)[0]
            for owner in range(per_chunk, owners_n, per_chunk)
        ),
        2 * quarter,
    ) if group_total > 1 else 2 * quarter
    pad = -(-(margin + slot_count) // 8) * 8
    return pl.pallas_call(
        functools.partial(assemble_kernel, owners_n, group_total, pad),
        out_shape=(
            jax.ShapeDtypeStruct((slot_count, width), jnp.bfloat16),
            jax.ShapeDtypeStruct((tokens_here, chunk), jnp.bfloat16),
        ),
        in_specs=[smem, vmem, vmem],
        out_specs=(vmem,) * 2,
        scratch_shapes=[pltpu.VMEM((chunk + 2 * pad, tokens_here), jnp.float32)],
        compiler_params=pltpu.CompilerParams(vmem_limit_bytes=VMEM_LIMIT),
        name="assemble",
    )(pltpu.with_memory_space_constraint(block_counts, pltpu.HBM), pieces, weight_grad)


def rotary_backward(key_grad, positions):
    tokens_here = key_grad.shape[0]
    half_dim = HD // 2
    cotangent = key_grad.astype(jnp.float32).reshape(tokens_here, -1, HD)
    freq_idx = jnp.arange(half_dim, dtype=jnp.float32)
    inverse = jnp.exp(-(2.0 * freq_idx / HD) * math.log(rope_base))
    angles = positions.astype(jnp.float32)[:, None] * inverse[None, :]
    cosine = jnp.cos(angles)[:, None, :]
    sine_part = jnp.sin(angles)[:, None, :]
    lower_half = cotangent[..., :half_dim]
    upper_half = cotangent[..., half_dim:]
    back_lower = lower_half * cosine + upper_half * sine_part
    back_upper = upper_half * cosine - lower_half * sine_part
    joined = jnp.concatenate([back_lower, back_upper], axis=-1)
    return joined.reshape(tokens_here, -1).astype(jnp.bfloat16)


def slot_tables(block_counts, slot_count, row_total):
    offsets = jnp.cumsum(block_counts) - block_counts
    owners_n = block_counts.shape[0]
    slot_ids = jnp.arange(owners_n * slot_count, dtype=jnp.int32)
    within = slot_ids % slot_count
    live_counts = jnp.broadcast_to(block_counts[:, None], (owners_n, slot_count)).reshape(-1)
    base_rows = jnp.broadcast_to(offsets[:, None], (owners_n, slot_count)).reshape(-1)
    is_live = within < live_counts
    row_of_slot = jnp.where(is_live, base_rows + within, 0)
    row_ids = jnp.arange(row_total, dtype=jnp.int32)
    at_or_after = row_ids[:, None] >= offsets[None, :]
    owner_of_row = jnp.sum(at_or_after.astype(jnp.int32), axis=1) - 1
    row_begin = jnp.max(jnp.where(at_or_after, offsets[None, :], 0), axis=1)
    slot_of_row = owner_of_row * slot_count + row_ids - row_begin
    return (row_of_slot, is_live, slot_of_row)


def gather_plan(hidden_in, key_grad, positions, key_quant, key_scales, block_counts):
    slot_count = key_quant.shape[0]
    local_heads = key_scales.shape[1]
    row_total = hidden_in.shape[1]
    row_of_slot, is_live, slot_of_row = slot_tables(block_counts, slot_count, row_total)
    scaled = (
        key_quant.astype(jnp.float32).reshape(slot_count, local_heads, HD) * key_scales[:, :, None]
    )
    local_weights = scaled.astype(jnp.bfloat16).reshape(slot_count, local_heads * HD)
    rotated = rotary_backward(key_grad, positions)
    picked = jnp.where(
        is_live[None, :], jnp.take(hidden_in, row_of_slot, axis=1), jnp.zeros((), jnp.bfloat16)
    )
    weight_grad = lax.psum_scatter(
        lax.dot_general(
            picked, rotated, (((0,), (0,)), ((), ())), preferred_element_type=jnp.float32
        ),
        "fsdp",
        scatter_dimension=0,
        tiled=True,
    ).astype(jnp.bfloat16)
    group_total = lax.axis_size("tp")
    whole_slots = lax.all_gather(local_weights, "fsdp", axis=0, tiled=True)
    ordered = jnp.take(whole_slots, slot_of_row, axis=0)
    own_rows = lax.all_to_all(ordered, "tp", split_axis=0, concat_axis=1, tiled=True)
    all_heads = lax.all_gather(rotated, "tp", axis=1, tiled=True)
    tokens_here = all_heads.shape[0]
    feature_here = own_rows.shape[0]
    heads_grouped = all_heads.reshape(tokens_here, group_total, -1)
    rows_grouped = own_rows.reshape(feature_here, group_total, -1)
    group_part = jnp.einsum(
        "tgk,dgk->gtd", heads_grouped, rows_grouped, preferred_element_type=jnp.float32
    ).astype(jnp.bfloat16)
    input_grad = jnp.sum(group_part.astype(jnp.float32), axis=0).astype(jnp.bfloat16)
    return (weight_grad, input_grad)


def per_device(hidden_in, key_grad, positions, key_quant, key_scales, block_counts):
    tokens_here, row_total = hidden_in.shape
    slot_count, width = key_quant.shape
    fits = exchange_fits(
        lax.axis_size("fsdp"), lax.axis_size("tp"), slot_count, row_total, tokens_here, width
    )
    plan = exchange_plan if fits else gather_plan
    return plan(hidden_in, key_grad, positions, key_quant, key_scales, block_counts)


def solution(mesh):
    in_specs = (P("fsdp", None), P("fsdp", "tp"), P("fsdp"), P("fsdp", "tp"), P("fsdp", "tp"), P())
    out_specs = (P("fsdp", "tp"), P("fsdp", "tp"))
    return jax.shard_map(
        per_device, mesh=mesh, in_specs=in_specs, out_specs=out_specs, check_vma=False
    )
```

```python
import functools
import math

import jax
import jax.numpy as jnp
from jax import lax
from jax.experimental import pallas as pl
from jax.experimental.pallas import tpu as pltpu
from jax.sharding import PartitionSpec as P

HD = 128
LANES = 128
LINE = 2
LOADS = 4
WRITES = 4
VMEM_LIMIT = 24 * 2**20
SIDE_CORE = 1
HIDE_AT = (1, 3)
WEIGH_FROM = (2, 1)
WEIGH_AT = 4
OUT_AT = 5
EARLY = 0
MESH = pl.DeviceIdType.MESH

rope_base = 500000.0


def offset_range(index, owners_n, row_total, slot_count):
    least_count = 2 * row_total // owners_n - slot_count
    later = owners_n - index
    least = max(index * least_count, row_total - later * slot_count)
    greatest = min(index * slot_count, row_total - later * least_count)
    return least, greatest


def exchange_fits(owners_n, group_total, slot_count, row_total, tokens_here, width):
    if group_total != 2 * LINE or owners_n % group_total or owners_n % LINE or slot_count % (16 * group_total):
        return False
    if tokens_here % LANES or width % LANES or row_total % group_total or (row_total // group_total) % (WRITES * LANES):
        return False
    quarter = slot_count // group_total
    chunk = row_total // group_total
    per_chunk = owners_n // group_total
    if 2 * row_total // owners_n - slot_count < quarter or row_total < 2 * quarter + 4 * LANES:
        return False
    for owner in range(owners_n):
        least, greatest = offset_range(owner, owners_n, row_total, slot_count)
        home = owner // per_chunk
        if greatest - least + quarter + 2 * LANES > row_total:
            return False
        for part in range(group_total):
            reach = range(
                max(0, (least + part * quarter) // chunk),
                min(group_total - 1, (greatest + (part + 1) * quarter - 1) // chunk) + 1,
            )
            allowed = {home}
            if part == 0 and owner % per_chunk == 0:
                allowed.add(home - 1)
            if part == group_total - 1 and owner % per_chunk == per_chunk - 1:
                allowed.add(home + 1)
            if not set(reach) <= allowed:
                return False
    return True


def assemble_kernel(
    owners_n, group_total, pad, counts_ref, pieces_ref, grad_ref, grad_out, input_out, rows, out_ref, sems
):
    chunk_at = lax.axis_index("tp")
    chunk = out_ref.shape[1]
    quarter = pieces_ref.shape[1]
    copies = []
    for part in range(group_total):
        copies.append(
            pltpu.make_async_copy(grad_ref.at[part], grad_out.at[pl.ds(part * quarter, quarter), :], sems.at[part])
        )
        copies[-1].start()
    per_chunk = owners_n // group_total
    offsets = []
    offset = jnp.int32(0)
    for owner in range(owners_n):
        offsets.append(offset)
        offset = offset + counts_ref[owner]

    def first_row(owner):
        found = jnp.int32(0)
        for candidate in range(owners_n):
            found = jnp.where(owner == candidate, offsets[candidate], found)
        return found

    limit = rows.shape[0] - quarter

    def place(index, begin):
        rows[pl.ds(jnp.clip(begin, 0, limit), quarter), :] = pieces_ref[index].astype(jnp.float32)

    origin = pad - chunk_at * chunk
    first = chunk_at * per_chunk
    below = first_row(first - 1) + (group_total - 1) * quarter + origin
    place(0, jnp.where(chunk_at > 0, below, 0))
    for near in range(per_chunk):
        start = first_row(first + near) + origin
        for part in range(group_total):
            place(1 + near * group_total + part, start + part * quarter)
    above = first_row(first + per_chunk) + origin
    last = 1 + per_chunk * group_total
    place(last, jnp.where(chunk_at < group_total - 1, above, limit))
    for at in range(0, chunk, LANES):
        out_ref[:, pl.ds(at, LANES)] = rows[pl.ds(pad + at, LANES), :].T.astype(jnp.bfloat16)
        if (at + LANES) % (chunk // WRITES) == 0:
            done = pl.ds(at + LANES - chunk // WRITES, chunk // WRITES)
            copies.append(pltpu.make_async_copy(out_ref.at[:, done], input_out.at[:, done], sems.at[len(copies)]))
            copies[-1].start()
    for copy in copies:
        copy.wait()


def exchange_kernel(
    owners_n, group_total, counts_ref, hidden_any, grad_any, positions_any, quant_any, scales_any,
    grad_out, pieces_out,
    hidden_in, grad_ref, positions_ref, quant_ref, scales_ref,
    weights_ref, rotated, weights, picked, hidden, outgoing, grad_send,
    load_sem, w_send, w_recv, h_send, h_recv,
    z_send, first_send, second_send, net_recv, pair_send, pair_recv,
    o_send, b_send, e_send, o_recv, g_send, g_recv,
    column_in, beside_in,
):
    here = lax.axis_index("fsdp")
    part = lax.axis_index("tp")
    core = lax.rem(part, 2)
    side = part // 2
    partner = part + 1 - 2 * core
    across = lax.rem(part + 2, group_total)
    tokens, width = grad_ref.shape
    row_total = hidden_in.shape[1]
    quarter = picked.shape[1]
    depth = owners_n // LINE
    z = here // LINE
    y = lax.rem(here, LINE)
    beside = z * LINE + (1 - y)
    per_chunk = owners_n // group_total
    home = here // per_chunk
    last_piece = 1 + per_chunk * group_total

    loads = [pltpu.make_async_copy(grad_any, grad_ref, load_sem.at[0])]
    loads.append(pltpu.make_async_copy(positions_any, positions_ref, load_sem.at[1]))
    columns_each = row_total // LOADS
    for at in range(LOADS):
        columns = pl.ds(at * columns_each, columns_each)
        loads.append(
            pltpu.make_async_copy(hidden_any.at[:, columns], hidden_in.at[:, columns], load_sem.at[4 + at])
        )
    loads.append(pltpu.make_async_copy(quant_any, quant_ref, load_sem.at[2]))
    loads.append(pltpu.make_async_copy(scales_any, scales_ref, load_sem.at[3]))
    for load in loads:
        load.start()
    barrier = pltpu.get_barrier_semaphore()

    def greet(where):
        pl.semaphore_signal(barrier, inc=1, device_id=where, device_id_type=MESH)

    @pl.when(z > 0)
    def _():
        greet((here - LINE, part))

    @pl.when(z < depth - 1)
    def _():
        greet((here + LINE, part))

    for row in range(LINE):
        for turn in range(group_total):
            if row or turn:
                greet((z * LINE + lax.rem(y + row, LINE), lax.rem(part + turn, group_total)))
    near_n = LINE * group_total - 1 + jnp.where(z > 0, 1, 0) + jnp.where(z < depth - 1, 1, 0)

    def remote(src, dst, send, recv, where):
        return pltpu.make_async_remote_copy(
            src_ref=src, dst_ref=dst, send_sem=send, recv_sem=recv, device_id=where, device_id_type=MESH
        )

    def rows_of(owner):
        return pl.ds(pl.multiple_of(owner * tokens, tokens), tokens)

    def cols_of(group):
        return pl.ds(pl.multiple_of(group * width, width), width)

    def slots_of(group):
        return pl.ds(pl.multiple_of(group * quarter, 16), quarter)

    peers = (lax.rem(partner + 2, group_total), across, partner)

    def weigh(kind):
        return remote(
            weights_ref.at[slots_of(peers[kind]), :], weights.at[:, cols_of(part)],
            w_send.at[kind], w_recv.at[kind], (here, peers[kind]),
        )

    def hide(target):
        return remote(
            picked.at[target], hidden.at[:, rows_of(here)],
            h_send.at[target], h_recv.at[here], (target, part),
        )

    def hidden_from(owner):
        return remote(
            picked.at[owner], hidden.at[:, rows_of(owner)],
            h_send.at[owner], h_recv.at[owner], (owner, part),
        )

    def block(owner, row, lane):
        return rotated.at[rows_of(owner), cols_of(2 * row + lane)]

    def relay(owner, row, send, where):
        view = block(owner, row, core)
        return remote(view, view, send, net_recv.at[owner * 2 + row], where)

    def share(owner, row, lane):
        view, at = block(owner, row, lane), owner * 2 + row
        return remote(view, view, pair_send.at[at], pair_recv.at[at], (here, partner))

    offsets = []
    offset = jnp.int32(0)
    for owner in range(owners_n):
        offsets.append(offset)
        offset = offset + counts_ref[owner]

    def pick(owner):
        least, greatest = offset_range(owner, owners_n, row_total, quarter * group_total)
        span = -(-(greatest - least + quarter + LANES) // LANES) * LANES
        base = jnp.minimum((least + part * quarter) // LANES * LANES, row_total - span)
        window = hidden_in[:, pl.ds(pl.multiple_of(base, LANES), span)]
        slot = lax.broadcasted_iota(jnp.int32, (quarter, span), 0)
        column = lax.broadcasted_iota(jnp.int32, (quarter, span), 1)
        first = offsets[owner] + part * quarter - base
        live = jnp.minimum(first + counts_ref[owner] - part * quarter, span)
        chosen = (column == slot + first) & (column < live)
        moved = lax.dot_general(
            chosen.astype(jnp.float32).astype(jnp.bfloat16), window, (((1,), (1,)), ((), ())),
            preferred_element_type=jnp.float32,
        )
        picked[owner] = moved.astype(jnp.bfloat16)

    loads[0].wait()
    loads[1].wait()
    heads = scales_ref.shape[0]
    lane = lax.broadcasted_iota(jnp.int32, (tokens, HD), 1)
    pair_at = jnp.where(lane < HD // 2, lane, lane - HD // 2).astype(jnp.float32)
    inverse = jnp.exp(-(2.0 * pair_at / HD) * math.log(rope_base))
    place = jnp.broadcast_to(positions_ref[...].astype(jnp.float32), (HD, tokens)).T
    angles = place * inverse
    cosine = jnp.cos(angles)
    sine = jnp.sin(angles)
    sine = jnp.where(lane < HD // 2, sine, -sine)
    for head in range(heads):
        values = grad_ref[:, pl.ds(head * HD, HD)].astype(jnp.float32)
        swapped = jnp.concatenate([values[:, HD // 2 :], values[:, : HD // 2]], axis=1)
        cols = pl.ds(pl.multiple_of(part * width + head * HD, HD), HD)
        rotated[rows_of(here), cols] = (values * cosine + swapped * sine).astype(jnp.bfloat16)
    with jax.named_scope("barrier"):
        pl.semaphore_wait(barrier, near_n)

    def begin(copy):
        copy.start()

    def finish(copy):
        copy.wait_send()

    def own_row(level):
        return level * LINE + y, side

    sideways = core == SIDE_CORE

    def first_row(level):
        return level * LINE + jnp.where(sideways, y, 1 - y), jnp.where(sideways, 1 - side, side)

    def second_row(level):
        return level * LINE + jnp.where(sideways, 1 - y, y), jnp.where(sideways, side, 1 - side)

    def last_row(level):
        return level * LINE + 1 - y, 1 - side

    first_to = (jnp.where(sideways, here, beside), jnp.where(sideways, across, part))
    second_to = (jnp.where(sideways, beside, here), jnp.where(sideways, part, across))

    def climb(level):
        return relay(*own_row(z), z_send.at[level], (level * LINE + y, part))

    def from_z(level, act):
        owner, row = own_row(level)
        act(relay(owner, row, first_send.at[owner], first_to))
        act(relay(owner, row, second_send.at[owner * 2 + row], second_to))
        act(share(owner, row, core))

    def from_first(level, act):
        owner, row = first_row(level)
        act(relay(owner, row, second_send.at[owner * 2 + row], second_to))
        act(share(owner, row, core))

    def from_second(level, act):
        act(share(*second_row(level), core))

    def from_last(level, act):
        act(share(*last_row(level), core))

    def arrived(owner, row):
        relay(owner, row, first_send.at[0], first_to).wait_recv()

    def levels(away):
        for sign in (-1, 1) if away else (1,):
            yield sign, z + sign * away

    def at_levels(away, act):
        if 0 <= away < depth:
            for sign, level in levels(away):

                @pl.when((level >= 0) & (level < depth))
                def _():
                    act(sign, level)

    def tell(level, known):
        pl.semaphore_signal(
            column_in.at[known], inc=1, device_id=(level * LINE + y, part), device_id_type=MESH
        )

    def heard(sign, known):
        @pl.when((z - sign >= 0) & (z - sign < depth))
        def _():
            tell(z - sign, known)

    at_levels(1, heard)
    at_levels(1, lambda sign, level: climb(level).start())
    from_z(z, begin)

    def farther(sign, level):
        pl.semaphore_wait(column_in.at[level], 1)
        heard(sign, level)
        climb(level).start()

    for away in range(2, depth):
        at_levels(away, farther)
    pl.semaphore_signal(beside_in, inc=1, device_id=(beside, part), device_id_type=MESH)
    for load in loads[2 : 2 + LOADS]:
        load.wait()
    for owner in range(owners_n):
        pick(owner)
    for load in loads[2 + LOADS :]:
        load.wait()
    for head in range(heads):
        cols = pl.ds(head * HD, HD)
        scale = jnp.broadcast_to(scales_ref[head : head + 1, :], (HD, scales_ref.shape[1])).T
        weights_ref[:, cols] = (quant_ref[:, cols].astype(jnp.float32) * scale).astype(jnp.bfloat16)
    weights[:, cols_of(part)] = weights_ref[slots_of(part), :]
    hidden[:, rows_of(here)] = picked[here]
    weigh(2).start()
    nearest = jnp.where(z > 0, z - 1, z + 1)
    hide(nearest * LINE + y).start()

    def hide_same(sign, level):
        @pl.when(level != nearest)
        def _():
            hide(level * LINE + y).start()

    def release(stage):
        if stage == HIDE_AT[0]:
            for away in range(1, depth):
                at_levels(away, hide_same)
        if stage == HIDE_AT[1]:
            pl.semaphore_wait(beside_in, 1)
            for away in range(1, depth):
                at_levels(away, lambda sign, level: hide(level * LINE + 1 - y).start())
            hide(beside).start()
        for kind, at in enumerate(WEIGH_FROM):
            if stage == at:
                weigh(kind).start()

    near = lax.rem(here, per_chunk)
    after_mine = (near == per_chunk - 1) & (part == group_total - 1) & (home < group_total - 1) & (lax.rem(home, 2) == 1)
    before_mine = (near == 0) & (part == 0) & (home > 0) & (lax.rem(home, 2) == 0)

    def send_piece(owner, act):
        source = outgoing.at[owner]
        index = 1 + lax.rem(here, per_chunk) * group_total + part
        mine = (owner == here) & (home == part)

        @pl.when(jnp.logical_not(mine))
        def _():
            act(remote(source, pieces_out.at[index], o_send.at[owner], o_recv.at[index], (owner, home)))

        @pl.when(after_mine)
        def _():
            act(remote(source, pieces_out.at[0], b_send.at[owner], o_recv.at[0], (owner, home + 1)))

        @pl.when(before_mine)
        def _():
            act(remote(source, pieces_out.at[last_piece], b_send.at[owner], o_recv.at[last_piece], (owner, home - 1)))

        if act is begin:

            @pl.when(mine)
            def _():
                pieces_out[index] = outgoing[owner]

    def produce(owner):
        with jax.named_scope("shared"):
            for row in range(2):
                share(owner, row, 1 - core).wait_recv()
        outgoing[owner] = lax.dot_general(
            weights[...], rotated[rows_of(owner), :], (((1,), (1,)), ((), ())),
            preferred_element_type=jnp.float32,
        ).astype(jnp.bfloat16)

    ready, made = [], []
    for stage in range(1, depth + 3):

        def take(name, row_of, pass_on):
            def act(sign, level):
                with jax.named_scope(f"{name}{stage}{sign}"):
                    arrived(*row_of(level))
                pass_on(sign, level)

            return act

        if stage < depth:
            at_levels(stage, take("z", own_row, lambda sign, level: from_z(level, begin)))
        at_levels(stage - 1, take("first", first_row, lambda sign, level: from_first(level, begin)))
        at_levels(stage - 1, take("second", second_row, lambda sign, level: from_second(level, begin)))
        at_levels(stage - 2, take("last", last_row, lambda sign, level: from_last(level, begin)))
        release(stage)
        if stage == WEIGH_AT:
            with jax.named_scope("weigh"):
                for kind in range(3):
                    weigh(kind).wait_recv()
        ready.append((stage - 1, y))
        ready.append((stage - 2, 1 - y))
        ready = [(away, row) for away, row in ready if 0 <= away < depth]
        if stage >= WEIGH_AT:
            due = None
            for away, row in ready:
                at_levels(away, lambda sign, level, row=row: produce(level * LINE + row))
                if due:
                    at_levels(due[0], lambda sign, level, row=due[1]: send_piece(level * LINE + row, begin))
                due = (away, row) if away <= EARLY else None
                if not due:
                    made.append((away, row))
            if due:
                made.append(due)
            ready = []
        if stage >= OUT_AT:
            for away, row in made[::-1]:
                at_levels(away, lambda sign, level, row=row: send_piece(level * LINE + row, begin))
            made = []

    with jax.named_scope("hidden"):
        for step in range(1, owners_n):
            hidden_from(lax.rem(here + step, owners_n)).wait_recv()

    def send_grad(kind):
        return remote(
            grad_send.at[peers[kind]], grad_out.at[part], g_send.at[kind], g_recv.at[kind], (here, peers[kind])
        )

    with jax.named_scope("reduce"):
        for kind, target in enumerate(peers + (part,)):
            grad_send[target] = jnp.dot(
                hidden[...], rotated[:, cols_of(target)], preferred_element_type=jnp.float32
            ).astype(jnp.bfloat16)
            if kind:
                send_grad(kind - 1).start()
    grad_out[part] = grad_send[part]

    for kind in range(3):
        weigh(kind).wait_send()
    for step in range(1, owners_n):
        hide(lax.rem(here + step, owners_n)).wait_send()
    for away in range(depth):
        if away:
            at_levels(away, lambda sign, level: climb(level).wait_send())
        at_levels(away, lambda sign, level: from_z(level, finish))
        at_levels(away, lambda sign, level: from_first(level, finish))
        at_levels(away, lambda sign, level: from_second(level, finish))
        at_levels(away, lambda sign, level: from_last(level, finish))

    mine_index = jnp.where(home == part, 1 + lax.rem(here, per_chunk) * group_total + part, 0)

    def landed(index):
        return remote(
            outgoing.at[0], pieces_out.at[index], o_send.at[0], o_recv.at[index], (here, partner)
        )

    def pass_on(index, to_chunk, slot, send):
        return remote(pieces_out.at[index], pieces_out.at[slot], e_send.at[send], o_recv.at[slot], (here, to_chunk))

    for index in (last_piece - 1, 1):

        @pl.when(mine_index != index)
        def _():
            with jax.named_scope("edge"):
                landed(index).wait_recv()

    @pl.when(core == 0)
    def _():
        pass_on(last_piece - 1, partner, 0, 0).start()

    @pl.when(core == 1)
    def _():
        pass_on(1, partner, last_piece, 1).start()

    for index in range(2, last_piece - 1):

        @pl.when(mine_index != index)
        def _():
            with jax.named_scope("landed"):
                landed(index).wait_recv()

    @pl.when(core == 0)
    def _():
        pass_on(last_piece - 1, partner, 0, 0).wait_send()

    @pl.when(core == 1)
    def _():
        pass_on(1, partner, last_piece, 1).wait_send()

    @pl.when(part < group_total - 1)
    def _():
        with jax.named_scope("above"):
            landed(last_piece).wait_recv()

    @pl.when(part > 0)
    def _():
        with jax.named_scope("below"):
            landed(0).wait_recv()

    for owner in range(owners_n):
        send_piece(jnp.int32(owner), finish)
    with jax.named_scope("grads"):
        for kind in range(3):
            send_grad(kind).wait_send()
            remote(grad_send.at[0], grad_out.at[0], g_send.at[kind], g_recv.at[kind], (here, partner)).wait_recv()


def exchange_plan(hidden_in, key_grad, positions, key_quant, key_scales, block_counts):
    owners_n = lax.axis_size("fsdp")
    group_total = lax.axis_size("tp")
    slot_count, width = key_quant.shape
    tokens_here, row_total = hidden_in.shape
    heads = key_scales.shape[1]
    quarter = slot_count // group_total
    chunk = row_total // group_total
    per_chunk = owners_n // group_total
    columns = width * group_total
    vmem = pl.BlockSpec(memory_space=pltpu.VMEM)
    anywhere = pl.BlockSpec(memory_space=pltpu.HBM)
    smem = pl.BlockSpec(memory_space=pltpu.SMEM)
    pieces_n = 2 + per_chunk * group_total
    dma = pltpu.SemaphoreType.DMA
    weight_grad, pieces = pl.pallas_call(
        functools.partial(exchange_kernel, owners_n, group_total),
        out_shape=(
            jax.ShapeDtypeStruct((group_total, quarter, width), jnp.bfloat16),
            jax.ShapeDtypeStruct((pieces_n, quarter, tokens_here), jnp.bfloat16),
        ),
        in_specs=[smem] + [anywhere] * 5,
        out_specs=(vmem,) * 2,
        scratch_shapes=[
            pltpu.VMEM((tokens_here, row_total), jnp.bfloat16),
            pltpu.VMEM((tokens_here, width), jnp.bfloat16),
            pltpu.VMEM((1, tokens_here), jnp.int32),
            pltpu.VMEM((slot_count, width), jnp.bfloat16),
            pltpu.VMEM((heads, slot_count), jnp.float32),
            pltpu.VMEM((slot_count, width), jnp.bfloat16),
            pltpu.VMEM((owners_n * tokens_here, columns), jnp.bfloat16),
            pltpu.VMEM((quarter, columns), jnp.bfloat16),
            pltpu.VMEM((owners_n, quarter, tokens_here), jnp.bfloat16),
            pltpu.VMEM((quarter, owners_n * tokens_here), jnp.bfloat16),
            pltpu.VMEM((owners_n, quarter, tokens_here), jnp.bfloat16),
            pltpu.VMEM((group_total, quarter, width), jnp.bfloat16),
            dma((4 + LOADS,)),
            dma((group_total - 1,)), dma((group_total - 1,)),
            dma((owners_n,)), dma((owners_n,)),
            dma((owners_n // LINE,)), dma((owners_n,)), dma((2 * owners_n,)), dma((2 * owners_n,)),
            dma((2 * owners_n,)), dma((2 * owners_n,)),
            dma((owners_n,)), dma((owners_n,)), dma((2,)), dma((pieces_n,)),
            dma((group_total - 1,)), dma((group_total - 1,)),
            pltpu.SemaphoreType.REGULAR((owners_n // LINE,)), pltpu.SemaphoreType.REGULAR,
        ],
        compiler_params=pltpu.CompilerParams(
            has_side_effects=True, collective_id=0, vmem_limit_bytes=VMEM_LIMIT
        ),
        name="exchange",
    )(*(
        pltpu.with_memory_space_constraint(array, pltpu.HBM)
        for array in (block_counts, hidden_in, key_grad, positions.reshape(1, -1), key_quant, key_scales.T)
    ))

    margin = max(
        max(
            chunk * (owner // per_chunk) - offset_range(owner - 1, owners_n, row_total, slot_count)[0]
            for owner in range(per_chunk, owners_n, per_chunk)
        ),
        2 * quarter,
    ) if group_total > 1 else 2 * quarter
    pad = -(-(margin + slot_count) // 8) * 8
    return pl.pallas_call(
        functools.partial(assemble_kernel, owners_n, group_total, pad),
        out_shape=(
            jax.ShapeDtypeStruct((slot_count, width), jnp.bfloat16),
            jax.ShapeDtypeStruct((tokens_here, chunk), jnp.bfloat16),
        ),
        in_specs=[smem, vmem, vmem],
        out_specs=(anywhere,) * 2,
        scratch_shapes=[
            pltpu.VMEM((chunk + 2 * pad, tokens_here), jnp.float32),
            pltpu.VMEM((tokens_here, chunk), jnp.bfloat16),
            dma((group_total + WRITES,)),
        ],
        compiler_params=pltpu.CompilerParams(vmem_limit_bytes=VMEM_LIMIT),
        name="assemble",
    )(pltpu.with_memory_space_constraint(block_counts, pltpu.HBM), pieces, weight_grad)


def rotary_backward(key_grad, positions):
    tokens_here = key_grad.shape[0]
    half_dim = HD // 2
    cotangent = key_grad.astype(jnp.float32).reshape(tokens_here, -1, HD)
    freq_idx = jnp.arange(half_dim, dtype=jnp.float32)
    inverse = jnp.exp(-(2.0 * freq_idx / HD) * math.log(rope_base))
    angles = positions.astype(jnp.float32)[:, None] * inverse[None, :]
    cosine = jnp.cos(angles)[:, None, :]
    sine_part = jnp.sin(angles)[:, None, :]
    lower_half = cotangent[..., :half_dim]
    upper_half = cotangent[..., half_dim:]
    back_lower = lower_half * cosine + upper_half * sine_part
    back_upper = upper_half * cosine - lower_half * sine_part
    joined = jnp.concatenate([back_lower, back_upper], axis=-1)
    return joined.reshape(tokens_here, -1).astype(jnp.bfloat16)


def slot_tables(block_counts, slot_count, row_total):
    offsets = jnp.cumsum(block_counts) - block_counts
    owners_n = block_counts.shape[0]
    slot_ids = jnp.arange(owners_n * slot_count, dtype=jnp.int32)
    within = slot_ids % slot_count
    live_counts = jnp.broadcast_to(block_counts[:, None], (owners_n, slot_count)).reshape(-1)
    base_rows = jnp.broadcast_to(offsets[:, None], (owners_n, slot_count)).reshape(-1)
    is_live = within < live_counts
    row_of_slot = jnp.where(is_live, base_rows + within, 0)
    row_ids = jnp.arange(row_total, dtype=jnp.int32)
    at_or_after = row_ids[:, None] >= offsets[None, :]
    owner_of_row = jnp.sum(at_or_after.astype(jnp.int32), axis=1) - 1
    row_begin = jnp.max(jnp.where(at_or_after, offsets[None, :], 0), axis=1)
    slot_of_row = owner_of_row * slot_count + row_ids - row_begin
    return (row_of_slot, is_live, slot_of_row)


def gather_plan(hidden_in, key_grad, positions, key_quant, key_scales, block_counts):
    slot_count = key_quant.shape[0]
    local_heads = key_scales.shape[1]
    row_total = hidden_in.shape[1]
    row_of_slot, is_live, slot_of_row = slot_tables(block_counts, slot_count, row_total)
    scaled = (
        key_quant.astype(jnp.float32).reshape(slot_count, local_heads, HD) * key_scales[:, :, None]
    )
    local_weights = scaled.astype(jnp.bfloat16).reshape(slot_count, local_heads * HD)
    rotated = rotary_backward(key_grad, positions)
    picked = jnp.where(
        is_live[None, :], jnp.take(hidden_in, row_of_slot, axis=1), jnp.zeros((), jnp.bfloat16)
    )
    weight_grad = lax.psum_scatter(
        lax.dot_general(
            picked, rotated, (((0,), (0,)), ((), ())), preferred_element_type=jnp.float32
        ),
        "fsdp",
        scatter_dimension=0,
        tiled=True,
    ).astype(jnp.bfloat16)
    group_total = lax.axis_size("tp")
    whole_slots = lax.all_gather(local_weights, "fsdp", axis=0, tiled=True)
    ordered = jnp.take(whole_slots, slot_of_row, axis=0)
    own_rows = lax.all_to_all(ordered, "tp", split_axis=0, concat_axis=1, tiled=True)
    all_heads = lax.all_gather(rotated, "tp", axis=1, tiled=True)
    tokens_here = all_heads.shape[0]
    feature_here = own_rows.shape[0]
    heads_grouped = all_heads.reshape(tokens_here, group_total, -1)
    rows_grouped = own_rows.reshape(feature_here, group_total, -1)
    group_part = jnp.einsum(
        "tgk,dgk->gtd", heads_grouped, rows_grouped, preferred_element_type=jnp.float32
    ).astype(jnp.bfloat16)
    input_grad = jnp.sum(group_part.astype(jnp.float32), axis=0).astype(jnp.bfloat16)
    return (weight_grad, input_grad)


def per_device(hidden_in, key_grad, positions, key_quant, key_scales, block_counts):
    tokens_here, row_total = hidden_in.shape
    slot_count, width = key_quant.shape
    fits = exchange_fits(
        lax.axis_size("fsdp"), lax.axis_size("tp"), slot_count, row_total, tokens_here, width
    )
    plan = exchange_plan if fits else gather_plan
    return plan(hidden_in, key_grad, positions, key_quant, key_scales, block_counts)


def solution(mesh):
    in_specs = (P("fsdp", None), P("fsdp", "tp"), P("fsdp"), P("fsdp", "tp"), P("fsdp", "tp"), P())
    out_specs = (P("fsdp", "tp"), P("fsdp", "tp"))
    return jax.shard_map(
        per_device, mesh=mesh, in_specs=in_specs, out_specs=out_specs, check_vma=False
    )
```

```python
import functools
import math

import jax
import jax.numpy as jnp
from jax import lax
from jax.experimental import pallas as pl
from jax.experimental.pallas import tpu as pltpu
from jax.sharding import PartitionSpec as P

HD = 128
LANES = 128
LINE = 2
LOADS = 4
WRITES = 4
VMEM_LIMIT = 24 * 2**20
SIDE_CORE = 1
HIDE_AT = (1, 3)
WEIGH_FROM = (3, 1)
WEIGH_AT = 4
OUT_AT = 5
EARLY = 0
FLUSH = -1
BESIDE_AT = 3
MESH = pl.DeviceIdType.MESH

rope_base = 500000.0


def offset_range(index, owners_n, row_total, slot_count):
    least_count = 2 * row_total // owners_n - slot_count
    later = owners_n - index
    least = max(index * least_count, row_total - later * slot_count)
    greatest = min(index * slot_count, row_total - later * least_count)
    return least, greatest


def exchange_fits(owners_n, group_total, slot_count, row_total, tokens_here, width):
    if group_total != 2 * LINE or owners_n % group_total or owners_n % LINE or slot_count % (16 * group_total):
        return False
    if tokens_here % LANES or width % LANES or row_total % group_total or (row_total // group_total) % (WRITES * LANES):
        return False
    quarter = slot_count // group_total
    chunk = row_total // group_total
    per_chunk = owners_n // group_total
    if 2 * row_total // owners_n - slot_count < quarter or row_total < 2 * quarter + 4 * LANES:
        return False
    for owner in range(owners_n):
        least, greatest = offset_range(owner, owners_n, row_total, slot_count)
        home = owner // per_chunk
        if greatest - least + quarter + 2 * LANES > row_total:
            return False
        for part in range(group_total):
            reach = range(
                max(0, (least + part * quarter) // chunk),
                min(group_total - 1, (greatest + (part + 1) * quarter - 1) // chunk) + 1,
            )
            allowed = {home}
            if part == 0 and owner % per_chunk == 0:
                allowed.add(home - 1)
            if part == group_total - 1 and owner % per_chunk == per_chunk - 1:
                allowed.add(home + 1)
            if not set(reach) <= allowed:
                return False
    return True


def assemble_kernel(
    owners_n, group_total, pad, counts_ref, pieces_ref, grad_ref, grad_out, input_out, rows, out_ref, sems
):
    chunk_at = lax.axis_index("tp")
    chunk = out_ref.shape[1]
    quarter = pieces_ref.shape[1]
    copies = []
    for part in range(group_total):
        copies.append(
            pltpu.make_async_copy(grad_ref.at[part], grad_out.at[pl.ds(part * quarter, quarter), :], sems.at[part])
        )
        copies[-1].start()
    per_chunk = owners_n // group_total
    offsets = []
    offset = jnp.int32(0)
    for owner in range(owners_n):
        offsets.append(offset)
        offset = offset + counts_ref[owner]

    def first_row(owner):
        found = jnp.int32(0)
        for candidate in range(owners_n):
            found = jnp.where(owner == candidate, offsets[candidate], found)
        return found

    limit = rows.shape[0] - quarter

    def place(index, begin):
        rows[pl.ds(jnp.clip(begin, 0, limit), quarter), :] = pieces_ref[index].astype(jnp.float32)

    origin = pad - chunk_at * chunk
    first = chunk_at * per_chunk
    below = first_row(first - 1) + (group_total - 1) * quarter + origin
    place(0, jnp.where(chunk_at > 0, below, 0))
    for near in range(per_chunk):
        start = first_row(first + near) + origin
        for part in range(group_total):
            place(1 + near * group_total + part, start + part * quarter)
    above = first_row(first + per_chunk) + origin
    last = 1 + per_chunk * group_total
    place(last, jnp.where(chunk_at < group_total - 1, above, limit))
    for at in range(0, chunk, LANES):
        out_ref[:, pl.ds(at, LANES)] = rows[pl.ds(pad + at, LANES), :].T.astype(jnp.bfloat16)
        if (at + LANES) % (chunk // WRITES) == 0:
            done = pl.ds(at + LANES - chunk // WRITES, chunk // WRITES)
            copies.append(pltpu.make_async_copy(out_ref.at[:, done], input_out.at[:, done], sems.at[len(copies)]))
            copies[-1].start()
    for copy in copies:
        copy.wait()


def exchange_kernel(
    owners_n, group_total, counts_ref, hidden_any, grad_any, positions_any, quant_any, scales_any,
    grad_out, pieces_out,
    hidden_in, grad_ref, positions_ref, quant_ref, scales_ref,
    weights_ref, rotated, weights, picked, hidden, outgoing, grad_send,
    load_sem, w_send, w_recv, h_send, h_recv,
    z_send, end_send, first_send, second_send, net_recv, pair_send, pair_recv,
    o_send, b_send, e_send, o_recv, g_send, g_recv,
    column_in, beside_in,
):
    here = lax.axis_index("fsdp")
    part = lax.axis_index("tp")
    core = lax.rem(part, 2)
    side = part // 2
    partner = part + 1 - 2 * core
    across = lax.rem(part + 2, group_total)
    tokens, width = grad_ref.shape
    row_total = hidden_in.shape[1]
    quarter = picked.shape[1]
    depth = owners_n // LINE
    z = here // LINE
    y = lax.rem(here, LINE)
    beside = z * LINE + (1 - y)
    per_chunk = owners_n // group_total
    home = here // per_chunk
    last_piece = 1 + per_chunk * group_total

    loads = [pltpu.make_async_copy(grad_any, grad_ref, load_sem.at[0])]
    loads.append(pltpu.make_async_copy(positions_any, positions_ref, load_sem.at[1]))
    columns_each = row_total // LOADS
    for at in range(LOADS):
        columns = pl.ds(at * columns_each, columns_each)
        loads.append(
            pltpu.make_async_copy(hidden_any.at[:, columns], hidden_in.at[:, columns], load_sem.at[4 + at])
        )
    loads.append(pltpu.make_async_copy(quant_any, quant_ref, load_sem.at[2]))
    loads.append(pltpu.make_async_copy(scales_any, scales_ref, load_sem.at[3]))
    for load in loads:
        load.start()
    barrier = pltpu.get_barrier_semaphore()

    def greet(where):
        pl.semaphore_signal(barrier, inc=1, device_id=where, device_id_type=MESH)

    @pl.when(z > 0)
    def _():
        greet((here - LINE, part))

    @pl.when(z < depth - 1)
    def _():
        greet((here + LINE, part))

    for row in range(LINE):
        for turn in range(group_total):
            if row or turn:
                greet((z * LINE + lax.rem(y + row, LINE), lax.rem(part + turn, group_total)))
    near_n = LINE * group_total - 1 + jnp.where(z > 0, 1, 0) + jnp.where(z < depth - 1, 1, 0)

    def remote(src, dst, send, recv, where):
        return pltpu.make_async_remote_copy(
            src_ref=src, dst_ref=dst, send_sem=send, recv_sem=recv, device_id=where, device_id_type=MESH
        )

    def rows_of(owner):
        return pl.ds(pl.multiple_of(owner * tokens, tokens), tokens)

    def cols_of(group):
        return pl.ds(pl.multiple_of(group * width, width), width)

    def slots_of(group):
        return pl.ds(pl.multiple_of(group * quarter, 16), quarter)

    peers = (lax.rem(partner + 2, group_total), across, partner)

    def weigh(kind):
        return remote(
            weights_ref.at[slots_of(peers[kind]), :], weights.at[:, cols_of(part)],
            w_send.at[kind], w_recv.at[kind], (here, peers[kind]),
        )

    def hide(target):
        return remote(
            picked.at[target], hidden.at[:, rows_of(here)],
            h_send.at[target], h_recv.at[here], (target, part),
        )

    def hidden_from(owner):
        return remote(
            picked.at[owner], hidden.at[:, rows_of(owner)],
            h_send.at[owner], h_recv.at[owner], (owner, part),
        )

    def block(owner, row, lane):
        return rotated.at[rows_of(owner), cols_of(2 * row + lane)]

    def relay(owner, row, send, where):
        view = block(owner, row, core)
        return remote(view, view, send, net_recv.at[owner * 2 + row], where)

    def share(owner, row, lane):
        view, at = block(owner, row, lane), owner * 2 + row
        return remote(view, view, pair_send.at[at], pair_recv.at[at], (here, partner))

    offsets = []
    offset = jnp.int32(0)
    for owner in range(owners_n):
        offsets.append(offset)
        offset = offset + counts_ref[owner]

    def pick(owner):
        least, greatest = offset_range(owner, owners_n, row_total, quarter * group_total)
        span = -(-(greatest - least + quarter + LANES) // LANES) * LANES
        base = jnp.minimum((least + part * quarter) // LANES * LANES, row_total - span)
        window = hidden_in[:, pl.ds(pl.multiple_of(base, LANES), span)]
        slot = lax.broadcasted_iota(jnp.int32, (quarter, span), 0)
        column = lax.broadcasted_iota(jnp.int32, (quarter, span), 1)
        first = offsets[owner] + part * quarter - base
        live = jnp.minimum(first + counts_ref[owner] - part * quarter, span)
        chosen = (column == slot + first) & (column < live)
        moved = lax.dot_general(
            chosen.astype(jnp.float32).astype(jnp.bfloat16), window, (((1,), (1,)), ((), ())),
            preferred_element_type=jnp.float32,
        )
        picked[owner] = moved.astype(jnp.bfloat16)

    loads[0].wait()
    loads[1].wait()
    heads = scales_ref.shape[0]
    lane = lax.broadcasted_iota(jnp.int32, (tokens, HD), 1)
    pair_at = jnp.where(lane < HD // 2, lane, lane - HD // 2).astype(jnp.float32)
    inverse = jnp.exp(-(2.0 * pair_at / HD) * math.log(rope_base))
    place = jnp.broadcast_to(positions_ref[...].astype(jnp.float32), (HD, tokens)).T
    angles = place * inverse
    cosine = jnp.cos(angles)
    sine = jnp.sin(angles)
    sine = jnp.where(lane < HD // 2, sine, -sine)
    for head in range(heads):
        values = grad_ref[:, pl.ds(head * HD, HD)].astype(jnp.float32)
        swapped = jnp.concatenate([values[:, HD // 2 :], values[:, : HD // 2]], axis=1)
        cols = pl.ds(pl.multiple_of(part * width + head * HD, HD), HD)
        rotated[rows_of(here), cols] = (values * cosine + swapped * sine).astype(jnp.bfloat16)
    with jax.named_scope("barrier"):
        pl.semaphore_wait(barrier, near_n)

    def begin(copy):
        copy.start()

    def finish(copy):
        copy.wait_send()

    def own_row(level):
        return level * LINE + y, side

    sideways = core >= SIDE_CORE

    def first_row(level):
        return level * LINE + jnp.where(sideways, y, 1 - y), jnp.where(sideways, 1 - side, side)

    def second_row(level):
        return level * LINE + jnp.where(sideways, 1 - y, y), jnp.where(sideways, side, 1 - side)

    def last_row(level):
        return level * LINE + 1 - y, 1 - side

    first_to = (jnp.where(sideways, here, beside), jnp.where(sideways, across, part))
    second_to = (jnp.where(sideways, beside, here), jnp.where(sideways, part, across))

    def climb(level):
        return relay(*own_row(z), z_send.at[level], (level * LINE + y, part))

    def from_z(level, act):
        owner, row = own_row(level)
        act(relay(owner, row, first_send.at[owner], first_to))
        act(relay(owner, row, second_send.at[owner * 2 + row], second_to))
        act(share(owner, row, core))

    def from_first(level, act):
        owner, row = first_row(level)
        act(relay(owner, row, second_send.at[owner * 2 + row], second_to))
        act(share(owner, row, core))

    def from_second(level, act):
        act(share(*second_row(level), core))

    def from_last(level, act):
        act(share(*last_row(level), core))

    def arrived(owner, row):
        relay(owner, row, first_send.at[0], first_to).wait_recv()

    def levels(away):
        for sign in (-1, 1) if away else (1,):
            yield sign, z + sign * away

    def at_levels(away, act):
        if 0 <= away < depth:
            for sign, level in levels(away):

                @pl.when((level >= 0) & (level < depth))
                def _():
                    act(sign, level)

    def climb_inside(level, act):
        @pl.when((level > 0) & (level < depth - 1))
        def _():
            act(climb(level))

    def feed_ends(level, act):
        @pl.when((z == 1) & (level > 1))
        def _():
            act(relay(*own_row(level), end_send.at[level], (y, part)))

        @pl.when((z == depth - 2) & (level < depth - 2))
        def _():
            act(relay(*own_row(level), end_send.at[level], ((depth - 1) * LINE + y, part)))

    def tell(level, known):
        pl.semaphore_signal(
            column_in.at[known], inc=1, device_id=(level * LINE + y, part), device_id_type=MESH
        )

    def heard(sign, known):
        @pl.when((z - sign >= 0) & (z - sign < depth))
        def _():
            tell(z - sign, known)

    at_levels(1, heard)
    at_levels(1, lambda sign, level: climb(level).start())
    from_z(z, begin)

    def farther(sign, level):
        pl.semaphore_wait(column_in.at[level], 1)
        heard(sign, level)
        climb_inside(level, begin)

    for away in range(2, depth):
        at_levels(away, farther)
    pl.semaphore_signal(beside_in, inc=1, device_id=(beside, part), device_id_type=MESH)
    for load in loads[2 : 2 + LOADS]:
        load.wait()
    for owner in range(owners_n):
        pick(owner)
    for load in loads[2 + LOADS :]:
        load.wait()
    for head in range(heads):
        cols = pl.ds(head * HD, HD)
        scale = jnp.broadcast_to(scales_ref[head : head + 1, :], (HD, scales_ref.shape[1])).T
        weights_ref[:, cols] = (quant_ref[:, cols].astype(jnp.float32) * scale).astype(jnp.bfloat16)
    weights[:, cols_of(part)] = weights_ref[slots_of(part), :]
    hidden[:, rows_of(here)] = picked[here]
    weigh(2).start()
    nearest = jnp.where(z > 0, z - 1, z + 1)
    hide(nearest * LINE + y).start()

    def hide_same(sign, level):
        @pl.when(level != nearest)
        def _():
            hide(level * LINE + y).start()

    def release(stage):
        if stage == HIDE_AT[0]:
            for away in range(1, depth):
                at_levels(away, hide_same)
        if stage == HIDE_AT[1]:
            pl.semaphore_wait(beside_in, 1)
            for away in range(1, depth):
                at_levels(away, lambda sign, level: hide(level * LINE + 1 - y).start())
        if stage == BESIDE_AT:
            hide(beside).start()
        for kind, at in enumerate(WEIGH_FROM):
            if stage == at:
                weigh(kind).start()

    near = lax.rem(here, per_chunk)
    after_mine = (near == per_chunk - 1) & (part == group_total - 1) & (home < group_total - 1) & (lax.rem(home, 2) == 1)
    before_mine = (near == 0) & (part == 0) & (home > 0) & (lax.rem(home, 2) == 0)

    def send_piece(owner, act):
        source = outgoing.at[owner]
        index = 1 + lax.rem(here, per_chunk) * group_total + part
        mine = (owner == here) & (home == part)

        @pl.when(jnp.logical_not(mine))
        def _():
            act(remote(source, pieces_out.at[index], o_send.at[owner], o_recv.at[index], (owner, home)))

        @pl.when(after_mine)
        def _():
            act(remote(source, pieces_out.at[0], b_send.at[owner], o_recv.at[0], (owner, home + 1)))

        @pl.when(before_mine)
        def _():
            act(remote(source, pieces_out.at[last_piece], b_send.at[owner], o_recv.at[last_piece], (owner, home - 1)))

        if act is begin:

            @pl.when(mine)
            def _():
                pieces_out[index] = outgoing[owner]

    def produce(owner):
        with jax.named_scope("shared"):
            for row in range(2):
                share(owner, row, 1 - core).wait_recv()
        outgoing[owner] = lax.dot_general(
            weights[...], rotated[rows_of(owner), :], (((1,), (1,)), ((), ())),
            preferred_element_type=jnp.float32,
        ).astype(jnp.bfloat16)

    ready, made = [], []
    for stage in range(1, depth + 3):

        def pass_z(sign, level):
            feed_ends(level, begin)
            from_z(level, begin)

        def take(name, row_of, pass_on):
            def act(sign, level):
                with jax.named_scope(f"{name}{stage}{sign}"):
                    arrived(*row_of(level))
                pass_on(sign, level)

            return act

        if stage < depth:
            at_levels(stage, take("z", own_row, pass_z))
        at_levels(stage - 1, take("first", first_row, lambda sign, level: from_first(level, begin)))
        at_levels(stage - 1, take("second", second_row, lambda sign, level: from_second(level, begin)))
        at_levels(stage - 2, take("last", last_row, lambda sign, level: from_last(level, begin)))
        release(stage)
        if stage == WEIGH_AT:
            with jax.named_scope("weigh"):
                for kind in range(3):
                    weigh(kind).wait_recv()
        ready.append((stage - 1, y))
        ready.append((stage - 2, 1 - y))
        ready = [(away, row) for away, row in ready if 0 <= away < depth]
        if stage >= WEIGH_AT:
            due = None
            for away, row in ready:
                at_levels(away, lambda sign, level, row=row: produce(level * LINE + row))
                if due:
                    at_levels(due[0], lambda sign, level, row=due[1]: send_piece(level * LINE + row, begin))
                due = (away, row) if away <= EARLY else None
                if not due:
                    made.append((away, row))
            if due:
                made.append(due)
            ready = []
        if stage >= OUT_AT:
            for away, row in made[::FLUSH]:
                at_levels(away, lambda sign, level, row=row: send_piece(level * LINE + row, begin))
            made = []

    with jax.named_scope("hidden"):
        for step in range(1, owners_n):
            hidden_from(lax.rem(here + step, owners_n)).wait_recv()

    def send_grad(kind):
        return remote(
            grad_send.at[peers[kind]], grad_out.at[part], g_send.at[kind], g_recv.at[kind], (here, peers[kind])
        )

    with jax.named_scope("reduce"):
        for kind, target in enumerate(peers + (part,)):
            grad_send[target] = jnp.dot(
                hidden[...], rotated[:, cols_of(target)], preferred_element_type=jnp.float32
            ).astype(jnp.bfloat16)
            if kind:
                send_grad(kind - 1).start()
    grad_out[part] = grad_send[part]

    for kind in range(3):
        weigh(kind).wait_send()
    for step in range(1, owners_n):
        hide(lax.rem(here + step, owners_n)).wait_send()
    for away in range(depth):
        if away == 1:
            at_levels(away, lambda sign, level: climb(level).wait_send())
        if away > 1:
            at_levels(away, lambda sign, level: climb_inside(level, finish))
        if away:
            at_levels(away, lambda sign, level: feed_ends(level, finish))
        at_levels(away, lambda sign, level: from_z(level, finish))
        at_levels(away, lambda sign, level: from_first(level, finish))
        at_levels(away, lambda sign, level: from_second(level, finish))
        at_levels(away, lambda sign, level: from_last(level, finish))

    mine_index = jnp.where(home == part, 1 + lax.rem(here, per_chunk) * group_total + part, 0)

    def landed(index):
        return remote(
            outgoing.at[0], pieces_out.at[index], o_send.at[0], o_recv.at[index], (here, partner)
        )

    def pass_on(index, to_chunk, slot, send):
        return remote(pieces_out.at[index], pieces_out.at[slot], e_send.at[send], o_recv.at[slot], (here, to_chunk))

    for index in (last_piece - 1, 1):

        @pl.when(mine_index != index)
        def _():
            with jax.named_scope("edge"):
                landed(index).wait_recv()

    @pl.when(core == 0)
    def _():
        pass_on(last_piece - 1, partner, 0, 0).start()

    @pl.when(core == 1)
    def _():
        pass_on(1, partner, last_piece, 1).start()

    for index in range(2, last_piece - 1):

        @pl.when(mine_index != index)
        def _():
            with jax.named_scope("landed"):
                landed(index).wait_recv()

    @pl.when(core == 0)
    def _():
        pass_on(last_piece - 1, partner, 0, 0).wait_send()

    @pl.when(core == 1)
    def _():
        pass_on(1, partner, last_piece, 1).wait_send()

    @pl.when(part < group_total - 1)
    def _():
        with jax.named_scope("above"):
            landed(last_piece).wait_recv()

    @pl.when(part > 0)
    def _():
        with jax.named_scope("below"):
            landed(0).wait_recv()

    for owner in range(owners_n):
        send_piece(jnp.int32(owner), finish)
    with jax.named_scope("grads"):
        for kind in range(3):
            send_grad(kind).wait_send()
            remote(grad_send.at[0], grad_out.at[0], g_send.at[kind], g_recv.at[kind], (here, partner)).wait_recv()


def exchange_plan(hidden_in, key_grad, positions, key_quant, key_scales, block_counts):
    owners_n = lax.axis_size("fsdp")
    group_total = lax.axis_size("tp")
    slot_count, width = key_quant.shape
    tokens_here, row_total = hidden_in.shape
    heads = key_scales.shape[1]
    quarter = slot_count // group_total
    chunk = row_total // group_total
    per_chunk = owners_n // group_total
    columns = width * group_total
    vmem = pl.BlockSpec(memory_space=pltpu.VMEM)
    anywhere = pl.BlockSpec(memory_space=pltpu.HBM)
    smem = pl.BlockSpec(memory_space=pltpu.SMEM)
    pieces_n = 2 + per_chunk * group_total
    dma = pltpu.SemaphoreType.DMA
    weight_grad, pieces = pl.pallas_call(
        functools.partial(exchange_kernel, owners_n, group_total),
        out_shape=(
            jax.ShapeDtypeStruct((group_total, quarter, width), jnp.bfloat16),
            jax.ShapeDtypeStruct((pieces_n, quarter, tokens_here), jnp.bfloat16),
        ),
        in_specs=[smem] + [anywhere] * 5,
        out_specs=(vmem,) * 2,
        scratch_shapes=[
            pltpu.VMEM((tokens_here, row_total), jnp.bfloat16),
            pltpu.VMEM((tokens_here, width), jnp.bfloat16),
            pltpu.VMEM((1, tokens_here), jnp.int32),
            pltpu.VMEM((slot_count, width), jnp.bfloat16),
            pltpu.VMEM((heads, slot_count), jnp.float32),
            pltpu.VMEM((slot_count, width), jnp.bfloat16),
            pltpu.VMEM((owners_n * tokens_here, columns), jnp.bfloat16),
            pltpu.VMEM((quarter, columns), jnp.bfloat16),
            pltpu.VMEM((owners_n, quarter, tokens_here), jnp.bfloat16),
            pltpu.VMEM((quarter, owners_n * tokens_here), jnp.bfloat16),
            pltpu.VMEM((owners_n, quarter, tokens_here), jnp.bfloat16),
            pltpu.VMEM((group_total, quarter, width), jnp.bfloat16),
            dma((4 + LOADS,)),
            dma((group_total - 1,)), dma((group_total - 1,)),
            dma((owners_n,)), dma((owners_n,)),
            dma((owners_n // LINE,)), dma((owners_n // LINE,)),
            dma((owners_n,)), dma((2 * owners_n,)), dma((2 * owners_n,)),
            dma((2 * owners_n,)), dma((2 * owners_n,)),
            dma((owners_n,)), dma((owners_n,)), dma((2,)), dma((pieces_n,)),
            dma((group_total - 1,)), dma((group_total - 1,)),
            pltpu.SemaphoreType.REGULAR((owners_n // LINE,)), pltpu.SemaphoreType.REGULAR,
        ],
        compiler_params=pltpu.CompilerParams(
            has_side_effects=True, collective_id=0, vmem_limit_bytes=VMEM_LIMIT
        ),
        name="exchange",
    )(*(
        pltpu.with_memory_space_constraint(array, pltpu.HBM)
        for array in (block_counts, hidden_in, key_grad, positions.reshape(1, -1), key_quant, key_scales.T)
    ))

    margin = max(
        max(
            chunk * (owner // per_chunk) - offset_range(owner - 1, owners_n, row_total, slot_count)[0]
            for owner in range(per_chunk, owners_n, per_chunk)
        ),
        2 * quarter,
    ) if group_total > 1 else 2 * quarter
    pad = -(-(margin + slot_count) // 8) * 8
    return pl.pallas_call(
        functools.partial(assemble_kernel, owners_n, group_total, pad),
        out_shape=(
            jax.ShapeDtypeStruct((slot_count, width), jnp.bfloat16),
            jax.ShapeDtypeStruct((tokens_here, chunk), jnp.bfloat16),
        ),
        in_specs=[smem, vmem, vmem],
        out_specs=(anywhere,) * 2,
        scratch_shapes=[
            pltpu.VMEM((chunk + 2 * pad, tokens_here), jnp.float32),
            pltpu.VMEM((tokens_here, chunk), jnp.bfloat16),
            dma((group_total + WRITES,)),
        ],
        compiler_params=pltpu.CompilerParams(vmem_limit_bytes=VMEM_LIMIT),
        name="assemble",
    )(pltpu.with_memory_space_constraint(block_counts, pltpu.HBM), pieces, weight_grad)


def rotary_backward(key_grad, positions):
    tokens_here = key_grad.shape[0]
    half_dim = HD // 2
    cotangent = key_grad.astype(jnp.float32).reshape(tokens_here, -1, HD)
    freq_idx = jnp.arange(half_dim, dtype=jnp.float32)
    inverse = jnp.exp(-(2.0 * freq_idx / HD) * math.log(rope_base))
    angles = positions.astype(jnp.float32)[:, None] * inverse[None, :]
    cosine = jnp.cos(angles)[:, None, :]
    sine_part = jnp.sin(angles)[:, None, :]
    lower_half = cotangent[..., :half_dim]
    upper_half = cotangent[..., half_dim:]
    back_lower = lower_half * cosine + upper_half * sine_part
    back_upper = upper_half * cosine - lower_half * sine_part
    joined = jnp.concatenate([back_lower, back_upper], axis=-1)
    return joined.reshape(tokens_here, -1).astype(jnp.bfloat16)


def slot_tables(block_counts, slot_count, row_total):
    offsets = jnp.cumsum(block_counts) - block_counts
    owners_n = block_counts.shape[0]
    slot_ids = jnp.arange(owners_n * slot_count, dtype=jnp.int32)
    within = slot_ids % slot_count
    live_counts = jnp.broadcast_to(block_counts[:, None], (owners_n, slot_count)).reshape(-1)
    base_rows = jnp.broadcast_to(offsets[:, None], (owners_n, slot_count)).reshape(-1)
    is_live = within < live_counts
    row_of_slot = jnp.where(is_live, base_rows + within, 0)
    row_ids = jnp.arange(row_total, dtype=jnp.int32)
    at_or_after = row_ids[:, None] >= offsets[None, :]
    owner_of_row = jnp.sum(at_or_after.astype(jnp.int32), axis=1) - 1
    row_begin = jnp.max(jnp.where(at_or_after, offsets[None, :], 0), axis=1)
    slot_of_row = owner_of_row * slot_count + row_ids - row_begin
    return (row_of_slot, is_live, slot_of_row)


def gather_plan(hidden_in, key_grad, positions, key_quant, key_scales, block_counts):
    slot_count = key_quant.shape[0]
    local_heads = key_scales.shape[1]
    row_total = hidden_in.shape[1]
    row_of_slot, is_live, slot_of_row = slot_tables(block_counts, slot_count, row_total)
    scaled = (
        key_quant.astype(jnp.float32).reshape(slot_count, local_heads, HD) * key_scales[:, :, None]
    )
    local_weights = scaled.astype(jnp.bfloat16).reshape(slot_count, local_heads * HD)
    rotated = rotary_backward(key_grad, positions)
    picked = jnp.where(
        is_live[None, :], jnp.take(hidden_in, row_of_slot, axis=1), jnp.zeros((), jnp.bfloat16)
    )
    weight_grad = lax.psum_scatter(
        lax.dot_general(
            picked, rotated, (((0,), (0,)), ((), ())), preferred_element_type=jnp.float32
        ),
        "fsdp",
        scatter_dimension=0,
        tiled=True,
    ).astype(jnp.bfloat16)
    group_total = lax.axis_size("tp")
    whole_slots = lax.all_gather(local_weights, "fsdp", axis=0, tiled=True)
    ordered = jnp.take(whole_slots, slot_of_row, axis=0)
    own_rows = lax.all_to_all(ordered, "tp", split_axis=0, concat_axis=1, tiled=True)
    all_heads = lax.all_gather(rotated, "tp", axis=1, tiled=True)
    tokens_here = all_heads.shape[0]
    feature_here = own_rows.shape[0]
    heads_grouped = all_heads.reshape(tokens_here, group_total, -1)
    rows_grouped = own_rows.reshape(feature_here, group_total, -1)
    group_part = jnp.einsum(
        "tgk,dgk->gtd", heads_grouped, rows_grouped, preferred_element_type=jnp.float32
    ).astype(jnp.bfloat16)
    input_grad = jnp.sum(group_part.astype(jnp.float32), axis=0).astype(jnp.bfloat16)
    return (weight_grad, input_grad)


def per_device(hidden_in, key_grad, positions, key_quant, key_scales, block_counts):
    tokens_here, row_total = hidden_in.shape
    slot_count, width = key_quant.shape
    fits = exchange_fits(
        lax.axis_size("fsdp"), lax.axis_size("tp"), slot_count, row_total, tokens_here, width
    )
    plan = exchange_plan if fits else gather_plan
    return plan(hidden_in, key_grad, positions, key_quant, key_scales, block_counts)


def solution(mesh):
    in_specs = (P("fsdp", None), P("fsdp", "tp"), P("fsdp"), P("fsdp", "tp"), P("fsdp", "tp"), P())
    out_specs = (P("fsdp", "tp"), P("fsdp", "tp"))
    return jax.shard_map(
        per_device, mesh=mesh, in_specs=in_specs, out_specs=out_specs, check_vma=False
    )
```

```python
import functools
import math

import jax
import jax.numpy as jnp
from jax import lax
from jax.experimental import pallas as pl
from jax.experimental.pallas import tpu as pltpu
from jax.sharding import PartitionSpec as P

HD = 128
LANES = 128
LINE = 2
LOADS = 4
WRITES = 4
VMEM_LIMIT = 24 * 2**20
SIDE_CORE = 1
HIDE_AT = (1, 3)
WEIGH_FROM = (3, 1)
WEIGH_AT = 4
OUT_AT = 5
EARLY = 0
FLUSH = -1
BESIDE_AT = 3
MESH = pl.DeviceIdType.MESH

rope_base = 500000.0


def offset_range(index, owners_n, row_total, slot_count):
    least_count = 2 * row_total // owners_n - slot_count
    later = owners_n - index
    least = max(index * least_count, row_total - later * slot_count)
    greatest = min(index * slot_count, row_total - later * least_count)
    return least, greatest


def exchange_fits(owners_n, group_total, slot_count, row_total, tokens_here, width):
    if group_total != 2 * LINE or owners_n % group_total or owners_n % LINE or slot_count % (16 * group_total):
        return False
    if tokens_here % LANES or width % LANES or row_total % group_total or (row_total // group_total) % (WRITES * LANES):
        return False
    quarter = slot_count // group_total
    chunk = row_total // group_total
    per_chunk = owners_n // group_total
    if 2 * row_total // owners_n - slot_count < quarter or row_total < 2 * quarter + 4 * LANES:
        return False
    for owner in range(owners_n):
        least, greatest = offset_range(owner, owners_n, row_total, slot_count)
        home = owner // per_chunk
        if greatest - least + quarter + 2 * LANES > row_total:
            return False
        for part in range(group_total):
            reach = range(
                max(0, (least + part * quarter) // chunk),
                min(group_total - 1, (greatest + (part + 1) * quarter - 1) // chunk) + 1,
            )
            allowed = {home}
            if part == 0 and owner % per_chunk == 0:
                allowed.add(home - 1)
            if part == group_total - 1 and owner % per_chunk == per_chunk - 1:
                allowed.add(home + 1)
            if not set(reach) <= allowed:
                return False
    return True


def assemble_kernel(
    owners_n, group_total, pad, counts_ref, pieces_ref, grad_ref, grad_out, input_out, rows, out_ref, sems
):
    chunk_at = lax.axis_index("tp")
    chunk = out_ref.shape[1]
    quarter = pieces_ref.shape[1]
    copies = []
    for part in range(group_total):
        copies.append(
            pltpu.make_async_copy(grad_ref.at[part], grad_out.at[pl.ds(part * quarter, quarter), :], sems.at[part])
        )
        copies[-1].start()
    per_chunk = owners_n // group_total
    offsets = []
    offset = jnp.int32(0)
    for owner in range(owners_n):
        offsets.append(offset)
        offset = offset + counts_ref[owner]

    def first_row(owner):
        found = jnp.int32(0)
        for candidate in range(owners_n):
            found = jnp.where(owner == candidate, offsets[candidate], found)
        return found

    limit = rows.shape[0] - quarter

    def place(index, begin):
        rows[pl.ds(jnp.clip(begin, 0, limit), quarter), :] = pieces_ref[index].astype(jnp.float32)

    origin = pad - chunk_at * chunk
    first = chunk_at * per_chunk
    below = first_row(first - 1) + (group_total - 1) * quarter + origin
    place(0, jnp.where(chunk_at > 0, below, 0))
    for near in range(per_chunk):
        start = first_row(first + near) + origin
        for part in range(group_total):
            place(1 + near * group_total + part, start + part * quarter)
    above = first_row(first + per_chunk) + origin
    last = 1 + per_chunk * group_total
    place(last, jnp.where(chunk_at < group_total - 1, above, limit))
    for at in range(0, chunk, LANES):
        out_ref[:, pl.ds(at, LANES)] = rows[pl.ds(pad + at, LANES), :].T.astype(jnp.bfloat16)
        if (at + LANES) % (chunk // WRITES) == 0:
            done = pl.ds(at + LANES - chunk // WRITES, chunk // WRITES)
            copies.append(pltpu.make_async_copy(out_ref.at[:, done], input_out.at[:, done], sems.at[len(copies)]))
            copies[-1].start()
    for copy in copies:
        copy.wait()


def exchange_kernel(
    owners_n, group_total, counts_ref, hidden_any, grad_any, positions_any, quant_any, scales_any,
    grad_out, pieces_out,
    hidden_in, grad_ref, positions_ref, quant_ref, scales_ref,
    weights_ref, rotated, weights, picked, hidden, outgoing, grad_send,
    load_sem, w_send, w_recv, h_send, h_recv,
    z_send, end_send, first_send, second_send, net_recv, pair_send, pair_recv,
    o_send, b_send, e_send, o_recv, g_send, g_recv,
    column_in, beside_in,
):
    here = lax.axis_index("fsdp")
    part = lax.axis_index("tp")
    core = lax.rem(part, 2)
    side = part // 2
    partner = part + 1 - 2 * core
    across = lax.rem(part + 2, group_total)
    tokens, width = grad_ref.shape
    row_total = hidden_in.shape[1]
    quarter = picked.shape[1]
    depth = owners_n // LINE
    z = here // LINE
    y = lax.rem(here, LINE)
    beside = z * LINE + (1 - y)
    per_chunk = owners_n // group_total
    home = here // per_chunk
    last_piece = 1 + per_chunk * group_total

    loads = [pltpu.make_async_copy(grad_any, grad_ref, load_sem.at[0])]
    loads.append(pltpu.make_async_copy(positions_any, positions_ref, load_sem.at[1]))
    columns_each = row_total // LOADS
    for at in range(LOADS):
        columns = pl.ds(at * columns_each, columns_each)
        loads.append(
            pltpu.make_async_copy(hidden_any.at[:, columns], hidden_in.at[:, columns], load_sem.at[4 + at])
        )
    loads.append(pltpu.make_async_copy(quant_any, quant_ref, load_sem.at[2]))
    loads.append(pltpu.make_async_copy(scales_any, scales_ref, load_sem.at[3]))
    for load in loads:
        load.start()
    barrier = pltpu.get_barrier_semaphore()

    def greet(where):
        pl.semaphore_signal(barrier, inc=1, device_id=where, device_id_type=MESH)

    @pl.when(z > 0)
    def _():
        greet((here - LINE, part))

    @pl.when(z < depth - 1)
    def _():
        greet((here + LINE, part))

    for row in range(LINE):
        for turn in range(group_total):
            if row or turn:
                greet((z * LINE + lax.rem(y + row, LINE), lax.rem(part + turn, group_total)))
    near_n = LINE * group_total - 1 + jnp.where(z > 0, 1, 0) + jnp.where(z < depth - 1, 1, 0)

    def remote(src, dst, send, recv, where):
        return pltpu.make_async_remote_copy(
            src_ref=src, dst_ref=dst, send_sem=send, recv_sem=recv, device_id=where, device_id_type=MESH
        )

    def rows_of(owner):
        return pl.ds(pl.multiple_of(owner * tokens, tokens), tokens)

    def cols_of(group):
        return pl.ds(pl.multiple_of(group * width, width), width)

    def slots_of(group):
        return pl.ds(pl.multiple_of(group * quarter, 16), quarter)

    peers = (lax.rem(partner + 2, group_total), across, partner)

    def weigh(kind):
        return remote(
            weights_ref.at[slots_of(peers[kind]), :], weights.at[:, cols_of(part)],
            w_send.at[kind], w_recv.at[kind], (here, peers[kind]),
        )

    def hide(target):
        return remote(
            picked.at[target], hidden.at[:, rows_of(here)],
            h_send.at[target], h_recv.at[here], (target, part),
        )

    def hidden_from(owner):
        return remote(
            picked.at[owner], hidden.at[:, rows_of(owner)],
            h_send.at[owner], h_recv.at[owner], (owner, part),
        )

    def block(owner, row, lane):
        return rotated.at[rows_of(owner), cols_of(2 * row + lane)]

    def relay(owner, row, send, where):
        view = block(owner, row, core)
        return remote(view, view, send, net_recv.at[owner * 2 + row], where)

    def share(owner, row, lane):
        view, at = block(owner, row, lane), owner * 2 + row
        return remote(view, view, pair_send.at[at], pair_recv.at[at], (here, partner))

    offsets = []
    offset = jnp.int32(0)
    for owner in range(owners_n):
        offsets.append(offset)
        offset = offset + counts_ref[owner]

    def pick(owner):
        least, greatest = offset_range(owner, owners_n, row_total, quarter * group_total)
        span = -(-(greatest - least + quarter + LANES) // LANES) * LANES
        base = jnp.minimum((least + part * quarter) // LANES * LANES, row_total - span)
        window = hidden_in[:, pl.ds(pl.multiple_of(base, LANES), span)]
        slot = lax.broadcasted_iota(jnp.int32, (quarter, span), 0)
        column = lax.broadcasted_iota(jnp.int32, (quarter, span), 1)
        first = offsets[owner] + part * quarter - base
        live = jnp.minimum(first + counts_ref[owner] - part * quarter, span)
        chosen = (column == slot + first) & (column < live)
        moved = lax.dot_general(
            chosen.astype(jnp.float32).astype(jnp.bfloat16), window, (((1,), (1,)), ((), ())),
            preferred_element_type=jnp.float32,
        )
        picked[owner] = moved.astype(jnp.bfloat16)

    loads[0].wait()
    loads[1].wait()
    heads = scales_ref.shape[0]
    lane = lax.broadcasted_iota(jnp.int32, (tokens, HD), 1)
    pair_at = jnp.where(lane < HD // 2, lane, lane - HD // 2).astype(jnp.float32)
    inverse = jnp.exp(-(2.0 * pair_at / HD) * math.log(rope_base))
    place = jnp.broadcast_to(positions_ref[...].astype(jnp.float32), (HD, tokens)).T
    angles = place * inverse
    cosine = jnp.cos(angles)
    sine = jnp.sin(angles)
    sine = jnp.where(lane < HD // 2, sine, -sine)
    for head in range(heads):
        values = grad_ref[:, pl.ds(head * HD, HD)].astype(jnp.float32)
        swapped = jnp.concatenate([values[:, HD // 2 :], values[:, : HD // 2]], axis=1)
        cols = pl.ds(pl.multiple_of(part * width + head * HD, HD), HD)
        rotated[rows_of(here), cols] = (values * cosine + swapped * sine).astype(jnp.bfloat16)
    with jax.named_scope("barrier"):
        pl.semaphore_wait(barrier, near_n)

    def begin(copy):
        copy.start()

    def finish(copy):
        copy.wait_send()

    def own_row(level):
        return level * LINE + y, side

    sideways = core >= SIDE_CORE

    def first_row(level):
        return level * LINE + jnp.where(sideways, y, 1 - y), jnp.where(sideways, 1 - side, side)

    def second_row(level):
        return level * LINE + jnp.where(sideways, 1 - y, y), jnp.where(sideways, side, 1 - side)

    def last_row(level):
        return level * LINE + 1 - y, 1 - side

    first_to = (jnp.where(sideways, here, beside), jnp.where(sideways, across, part))
    second_to = (jnp.where(sideways, beside, here), jnp.where(sideways, part, across))

    def climb(level):
        return relay(*own_row(z), z_send.at[level], (level * LINE + y, part))

    def from_z(level, act):
        owner, row = own_row(level)
        act(relay(owner, row, first_send.at[owner], first_to))
        act(relay(owner, row, second_send.at[owner * 2 + row], second_to))
        act(share(owner, row, core))

    def from_first(level, act):
        owner, row = first_row(level)
        act(relay(owner, row, second_send.at[owner * 2 + row], second_to))
        act(share(owner, row, core))

    def from_second(level, act):
        act(share(*second_row(level), core))

    def from_last(level, act):
        act(share(*last_row(level), core))

    def arrived(owner, row):
        relay(owner, row, first_send.at[0], first_to).wait_recv()

    def levels(away):
        for sign in (-1, 1) if away else (1,):
            yield sign, z + sign * away

    def at_levels(away, act):
        if 0 <= away < depth:
            for sign, level in levels(away):

                @pl.when((level >= 0) & (level < depth))
                def _():
                    act(sign, level)

    def climb_inside(level, act):
        @pl.when((level > 0) & (level < depth - 1))
        def _():
            act(climb(level))

    def feed_ends(level, act):
        @pl.when((z == 1) & (level > 1))
        def _():
            act(relay(*own_row(level), end_send.at[level], (y, part)))

        @pl.when((z == depth - 2) & (level < depth - 2))
        def _():
            act(relay(*own_row(level), end_send.at[level], ((depth - 1) * LINE + y, part)))

    def tell(level, known):
        pl.semaphore_signal(
            column_in.at[known], inc=1, device_id=(level * LINE + y, part), device_id_type=MESH
        )

    def heard(sign, known):
        @pl.when((z - sign >= 0) & (z - sign < depth))
        def _():
            tell(z - sign, known)

    at_levels(1, heard)
    at_levels(1, lambda sign, level: climb(level).start())
    from_z(z, begin)

    def farther(sign, level):
        pl.semaphore_wait(column_in.at[level], 1)
        heard(sign, level)
        climb_inside(level, begin)

    for away in range(2, depth):
        at_levels(away, farther)
    pl.semaphore_signal(beside_in, inc=1, device_id=(beside, part), device_id_type=MESH)
    for load in loads[2 : 2 + LOADS]:
        load.wait()
    for owner in range(owners_n):
        pick(owner)
    for load in loads[2 + LOADS :]:
        load.wait()
    for head in range(heads):
        cols = pl.ds(head * HD, HD)
        scale = jnp.broadcast_to(scales_ref[head : head + 1, :], (HD, scales_ref.shape[1])).T
        weights_ref[:, cols] = (quant_ref[:, cols].astype(jnp.float32) * scale).astype(jnp.bfloat16)
    weights[:, cols_of(part)] = weights_ref[slots_of(part), :]
    hidden[:, rows_of(here)] = picked[here]
    weigh(2).start()
    nearest = jnp.where(z > 0, z - 1, z + 1)
    hide(nearest * LINE + y).start()

    def hide_same(sign, level):
        @pl.when(level != nearest)
        def _():
            hide(level * LINE + y).start()

    def release(stage):
        if stage == HIDE_AT[0]:
            for away in range(1, depth):
                at_levels(away, hide_same)
        if stage == HIDE_AT[1]:
            pl.semaphore_wait(beside_in, 1)
            for away in range(1, depth):
                at_levels(away, lambda sign, level: hide(level * LINE + 1 - y).start())
        if stage == BESIDE_AT:
            hide(beside).start()
        for kind, at in enumerate(WEIGH_FROM):
            if stage == at:
                weigh(kind).start()

    near = lax.rem(here, per_chunk)
    after_mine = (near == per_chunk - 1) & (part == group_total - 1) & (home < group_total - 1) & (lax.rem(home, 2) == 1)
    before_mine = (near == 0) & (part == 0) & (home > 0) & (lax.rem(home, 2) == 0)

    def send_piece(owner, act):
        source = outgoing.at[owner]
        index = 1 + lax.rem(here, per_chunk) * group_total + part
        mine = (owner == here) & (home == part)

        @pl.when(jnp.logical_not(mine))
        def _():
            act(remote(source, pieces_out.at[index], o_send.at[owner], o_recv.at[index], (owner, home)))

        @pl.when(after_mine)
        def _():
            act(remote(source, pieces_out.at[0], b_send.at[owner], o_recv.at[0], (owner, home + 1)))

        @pl.when(before_mine)
        def _():
            act(remote(source, pieces_out.at[last_piece], b_send.at[owner], o_recv.at[last_piece], (owner, home - 1)))

        if act is begin:

            @pl.when(mine)
            def _():
                pieces_out[index] = outgoing[owner]

    def produce(owner):
        with jax.named_scope("shared"):
            for row in range(2):
                share(owner, row, 1 - core).wait_recv()
        outgoing[owner] = lax.dot_general(
            weights[...], rotated[rows_of(owner), :], (((1,), (1,)), ((), ())),
            preferred_element_type=jnp.float32,
        ).astype(jnp.bfloat16)

    ready, made = [], []
    for stage in range(1, depth + 3):

        def pass_z(sign, level):
            feed_ends(level, begin)
            from_z(level, begin)

        def take(name, row_of, pass_on):
            def act(sign, level):
                with jax.named_scope(f"{name}{stage}{sign}"):
                    arrived(*row_of(level))
                pass_on(sign, level)

            return act

        if stage < depth:
            at_levels(stage, take("z", own_row, pass_z))
        at_levels(stage - 1, take("first", first_row, lambda sign, level: from_first(level, begin)))
        at_levels(stage - 1, take("second", second_row, lambda sign, level: from_second(level, begin)))
        at_levels(stage - 2, take("last", last_row, lambda sign, level: from_last(level, begin)))
        release(stage)
        if stage == WEIGH_AT:
            with jax.named_scope("weigh"):
                for kind in range(3):
                    weigh(kind).wait_recv()
        ready.append((stage - 1, y))
        ready.append((stage - 2, 1 - y))
        ready = [(away, row) for away, row in ready if 0 <= away < depth]
        if stage >= WEIGH_AT:
            due = None
            for away, row in ready:
                at_levels(away, lambda sign, level, row=row: produce(level * LINE + row))
                if due:
                    at_levels(due[0], lambda sign, level, row=due[1]: send_piece(level * LINE + row, begin))
                due = (away, row) if away <= EARLY else None
                if not due:
                    made.append((away, row))
            if due:
                made.append(due)
            ready = []
        if stage >= OUT_AT:
            for away, row in made[::FLUSH]:
                at_levels(away, lambda sign, level, row=row: send_piece(level * LINE + row, begin))
            made = []

    with jax.named_scope("hidden"):
        for step in range(1, owners_n):
            hidden_from(lax.rem(here + step, owners_n)).wait_recv()

    upper = (quarter // 2 + 15) // 16 * 16
    halves = (pl.ds(0, upper), pl.ds(upper, quarter - upper))

    def send_grad(kind, half):
        at, rows = kind * 2 + half, halves[half]
        return remote(
            grad_send.at[peers[kind], rows, :], grad_out.at[part, rows, :], g_send.at[at], g_recv.at[at],
            (here, peers[kind]),
        )

    pieces = [(kind, half) for kind in range(3) for half in range(2)]
    with jax.named_scope("reduce"):
        for step, (kind, half) in enumerate(pieces + [(3, 0), (3, 1)]):
            target = (peers + (part,))[kind]
            grad_send[target, halves[half], :] = jnp.dot(
                hidden[halves[half], :], rotated[:, cols_of(target)], preferred_element_type=jnp.float32
            ).astype(jnp.bfloat16)
            if 0 < step <= len(pieces):
                send_grad(*pieces[step - 1]).start()
    grad_out[part] = grad_send[part]

    for kind in range(3):
        weigh(kind).wait_send()
    for step in range(1, owners_n):
        hide(lax.rem(here + step, owners_n)).wait_send()
    for away in range(depth):
        if away == 1:
            at_levels(away, lambda sign, level: climb(level).wait_send())
        if away > 1:
            at_levels(away, lambda sign, level: climb_inside(level, finish))
        if away:
            at_levels(away, lambda sign, level: feed_ends(level, finish))
        at_levels(away, lambda sign, level: from_z(level, finish))
        at_levels(away, lambda sign, level: from_first(level, finish))
        at_levels(away, lambda sign, level: from_second(level, finish))
        at_levels(away, lambda sign, level: from_last(level, finish))

    mine_index = jnp.where(home == part, 1 + lax.rem(here, per_chunk) * group_total + part, 0)

    def landed(index):
        return remote(
            outgoing.at[0], pieces_out.at[index], o_send.at[0], o_recv.at[index], (here, partner)
        )

    def pass_on(index, to_chunk, slot, send):
        return remote(pieces_out.at[index], pieces_out.at[slot], e_send.at[send], o_recv.at[slot], (here, to_chunk))

    for index in (last_piece - 1, 1):

        @pl.when(mine_index != index)
        def _():
            with jax.named_scope("edge"):
                landed(index).wait_recv()

    @pl.when(core == 0)
    def _():
        pass_on(last_piece - 1, partner, 0, 0).start()

    @pl.when(core == 1)
    def _():
        pass_on(1, partner, last_piece, 1).start()

    for index in range(2, last_piece - 1):

        @pl.when(mine_index != index)
        def _():
            with jax.named_scope("landed"):
                landed(index).wait_recv()

    @pl.when(core == 0)
    def _():
        pass_on(last_piece - 1, partner, 0, 0).wait_send()

    @pl.when(core == 1)
    def _():
        pass_on(1, partner, last_piece, 1).wait_send()

    @pl.when(part < group_total - 1)
    def _():
        with jax.named_scope("above"):
            landed(last_piece).wait_recv()

    @pl.when(part > 0)
    def _():
        with jax.named_scope("below"):
            landed(0).wait_recv()

    for owner in range(owners_n):
        send_piece(jnp.int32(owner), finish)
    with jax.named_scope("grads"):
        for kind, half in pieces:
            send_grad(kind, half).wait_send()
            send_grad(kind, half).wait_recv()


def exchange_plan(hidden_in, key_grad, positions, key_quant, key_scales, block_counts):
    owners_n = lax.axis_size("fsdp")
    group_total = lax.axis_size("tp")
    slot_count, width = key_quant.shape
    tokens_here, row_total = hidden_in.shape
    heads = key_scales.shape[1]
    quarter = slot_count // group_total
    chunk = row_total // group_total
    per_chunk = owners_n // group_total
    columns = width * group_total
    vmem = pl.BlockSpec(memory_space=pltpu.VMEM)
    anywhere = pl.BlockSpec(memory_space=pltpu.HBM)
    smem = pl.BlockSpec(memory_space=pltpu.SMEM)
    pieces_n = 2 + per_chunk * group_total
    dma = pltpu.SemaphoreType.DMA
    weight_grad, pieces = pl.pallas_call(
        functools.partial(exchange_kernel, owners_n, group_total),
        out_shape=(
            jax.ShapeDtypeStruct((group_total, quarter, width), jnp.bfloat16),
            jax.ShapeDtypeStruct((pieces_n, quarter, tokens_here), jnp.bfloat16),
        ),
        in_specs=[smem] + [anywhere] * 5,
        out_specs=(vmem,) * 2,
        scratch_shapes=[
            pltpu.VMEM((tokens_here, row_total), jnp.bfloat16),
            pltpu.VMEM((tokens_here, width), jnp.bfloat16),
            pltpu.VMEM((1, tokens_here), jnp.int32),
            pltpu.VMEM((slot_count, width), jnp.bfloat16),
            pltpu.VMEM((heads, slot_count), jnp.float32),
            pltpu.VMEM((slot_count, width), jnp.bfloat16),
            pltpu.VMEM((owners_n * tokens_here, columns), jnp.bfloat16),
            pltpu.VMEM((quarter, columns), jnp.bfloat16),
            pltpu.VMEM((owners_n, quarter, tokens_here), jnp.bfloat16),
            pltpu.VMEM((quarter, owners_n * tokens_here), jnp.bfloat16),
            pltpu.VMEM((owners_n, quarter, tokens_here), jnp.bfloat16),
            pltpu.VMEM((group_total, quarter, width), jnp.bfloat16),
            dma((4 + LOADS,)),
            dma((group_total - 1,)), dma((group_total - 1,)),
            dma((owners_n,)), dma((owners_n,)),
            dma((owners_n // LINE,)), dma((owners_n // LINE,)),
            dma((owners_n,)), dma((2 * owners_n,)), dma((2 * owners_n,)),
            dma((2 * owners_n,)), dma((2 * owners_n,)),
            dma((owners_n,)), dma((owners_n,)), dma((2,)), dma((pieces_n,)),
            dma((2 * group_total - 2,)), dma((2 * group_total - 2,)),
            pltpu.SemaphoreType.REGULAR((owners_n // LINE,)), pltpu.SemaphoreType.REGULAR,
        ],
        compiler_params=pltpu.CompilerParams(
            has_side_effects=True, collective_id=0, vmem_limit_bytes=VMEM_LIMIT
        ),
        name="exchange",
    )(*(
        pltpu.with_memory_space_constraint(array, pltpu.HBM)
        for array in (block_counts, hidden_in, key_grad, positions.reshape(1, -1), key_quant, key_scales.T)
    ))

    margin = max(
        max(
            chunk * (owner // per_chunk) - offset_range(owner - 1, owners_n, row_total, slot_count)[0]
            for owner in range(per_chunk, owners_n, per_chunk)
        ),
        2 * quarter,
    ) if group_total > 1 else 2 * quarter
    pad = -(-(margin + slot_count) // 8) * 8
    return pl.pallas_call(
        functools.partial(assemble_kernel, owners_n, group_total, pad),
        out_shape=(
            jax.ShapeDtypeStruct((slot_count, width), jnp.bfloat16),
            jax.ShapeDtypeStruct((tokens_here, chunk), jnp.bfloat16),
        ),
        in_specs=[smem, vmem, vmem],
        out_specs=(anywhere,) * 2,
        scratch_shapes=[
            pltpu.VMEM((chunk + 2 * pad, tokens_here), jnp.float32),
            pltpu.VMEM((tokens_here, chunk), jnp.bfloat16),
            dma((group_total + WRITES,)),
        ],
        compiler_params=pltpu.CompilerParams(vmem_limit_bytes=VMEM_LIMIT),
        name="assemble",
    )(pltpu.with_memory_space_constraint(block_counts, pltpu.HBM), pieces, weight_grad)


def rotary_backward(key_grad, positions):
    tokens_here = key_grad.shape[0]
    half_dim = HD // 2
    cotangent = key_grad.astype(jnp.float32).reshape(tokens_here, -1, HD)
    freq_idx = jnp.arange(half_dim, dtype=jnp.float32)
    inverse = jnp.exp(-(2.0 * freq_idx / HD) * math.log(rope_base))
    angles = positions.astype(jnp.float32)[:, None] * inverse[None, :]
    cosine = jnp.cos(angles)[:, None, :]
    sine_part = jnp.sin(angles)[:, None, :]
    lower_half = cotangent[..., :half_dim]
    upper_half = cotangent[..., half_dim:]
    back_lower = lower_half * cosine + upper_half * sine_part
    back_upper = upper_half * cosine - lower_half * sine_part
    joined = jnp.concatenate([back_lower, back_upper], axis=-1)
    return joined.reshape(tokens_here, -1).astype(jnp.bfloat16)


def slot_tables(block_counts, slot_count, row_total):
    offsets = jnp.cumsum(block_counts) - block_counts
    owners_n = block_counts.shape[0]
    slot_ids = jnp.arange(owners_n * slot_count, dtype=jnp.int32)
    within = slot_ids % slot_count
    live_counts = jnp.broadcast_to(block_counts[:, None], (owners_n, slot_count)).reshape(-1)
    base_rows = jnp.broadcast_to(offsets[:, None], (owners_n, slot_count)).reshape(-1)
    is_live = within < live_counts
    row_of_slot = jnp.where(is_live, base_rows + within, 0)
    row_ids = jnp.arange(row_total, dtype=jnp.int32)
    at_or_after = row_ids[:, None] >= offsets[None, :]
    owner_of_row = jnp.sum(at_or_after.astype(jnp.int32), axis=1) - 1
    row_begin = jnp.max(jnp.where(at_or_after, offsets[None, :], 0), axis=1)
    slot_of_row = owner_of_row * slot_count + row_ids - row_begin
    return (row_of_slot, is_live, slot_of_row)


def gather_plan(hidden_in, key_grad, positions, key_quant, key_scales, block_counts):
    slot_count = key_quant.shape[0]
    local_heads = key_scales.shape[1]
    row_total = hidden_in.shape[1]
    row_of_slot, is_live, slot_of_row = slot_tables(block_counts, slot_count, row_total)
    scaled = (
        key_quant.astype(jnp.float32).reshape(slot_count, local_heads, HD) * key_scales[:, :, None]
    )
    local_weights = scaled.astype(jnp.bfloat16).reshape(slot_count, local_heads * HD)
    rotated = rotary_backward(key_grad, positions)
    picked = jnp.where(
        is_live[None, :], jnp.take(hidden_in, row_of_slot, axis=1), jnp.zeros((), jnp.bfloat16)
    )
    weight_grad = lax.psum_scatter(
        lax.dot_general(
            picked, rotated, (((0,), (0,)), ((), ())), preferred_element_type=jnp.float32
        ),
        "fsdp",
        scatter_dimension=0,
        tiled=True,
    ).astype(jnp.bfloat16)
    group_total = lax.axis_size("tp")
    whole_slots = lax.all_gather(local_weights, "fsdp", axis=0, tiled=True)
    ordered = jnp.take(whole_slots, slot_of_row, axis=0)
    own_rows = lax.all_to_all(ordered, "tp", split_axis=0, concat_axis=1, tiled=True)
    all_heads = lax.all_gather(rotated, "tp", axis=1, tiled=True)
    tokens_here = all_heads.shape[0]
    feature_here = own_rows.shape[0]
    heads_grouped = all_heads.reshape(tokens_here, group_total, -1)
    rows_grouped = own_rows.reshape(feature_here, group_total, -1)
    group_part = jnp.einsum(
        "tgk,dgk->gtd", heads_grouped, rows_grouped, preferred_element_type=jnp.float32
    ).astype(jnp.bfloat16)
    input_grad = jnp.sum(group_part.astype(jnp.float32), axis=0).astype(jnp.bfloat16)
    return (weight_grad, input_grad)


def per_device(hidden_in, key_grad, positions, key_quant, key_scales, block_counts):
    tokens_here, row_total = hidden_in.shape
    slot_count, width = key_quant.shape
    fits = exchange_fits(
        lax.axis_size("fsdp"), lax.axis_size("tp"), slot_count, row_total, tokens_here, width
    )
    plan = exchange_plan if fits else gather_plan
    return plan(hidden_in, key_grad, positions, key_quant, key_scales, block_counts)


def solution(mesh):
    in_specs = (P("fsdp", None), P("fsdp", "tp"), P("fsdp"), P("fsdp", "tp"), P("fsdp", "tp"), P())
    out_specs = (P("fsdp", "tp"), P("fsdp", "tp"))
    return jax.shard_map(
        per_device, mesh=mesh, in_specs=in_specs, out_specs=out_specs, check_vma=False
    )
```
